32 devices in a mesh: box: 4 (over x, core), dir: 8 (over z, y).
Axes of the slice: x: 2, y: 2, z: 4, core: 2. Of those that a mesh axis runs over, the one named last changes fastest.
Arguments:
- fine_out: float32 [2, 512, 4096], P(None, 'box', 'dir'), may hold values from -6 to 6
- interp_index: int32 [16384, 4], P('dir'), may hold values from 0 to 4095, as said below
- interp_weight: float32 [16384, 4], P('dir'), may hold values from 0.05 to 0.5
- child_angle: float32 [4, 16384], P(None, 'dir'), may hold values from -3.140625 to 3.140625
- translator: float32 [2, 316, 16384], P(None, None, 'dir'), may hold values from -4 to 4
- partners: int32 [128, 30], P('box'), may hold values from 0 to 127, as said below
- offsets: int32 [128, 30], P('box'), may hold values from 0 to 315
- list_count: int32 [128], P('box'), may hold values from 15 to 30
Outputs:
- fine_in: float32 [2, 512, 4096], P(None, 'box', 'dir')
The draws below stay inside these ranges and needn't reach their ends.
Inputs may be any that keep to these rules, and one draw needn't show every extreme that they name: `interp_index`: for parent sample j = (a, b) every entry is a child sample (theta, phi) with theta within 1 of a // 2 and phi within 2 of b // 2 counted around the phi circle; both distances are reached. `partners`: every entry lies within 16 of its row number b, is not b, and the distance 16 is reached.
All inputs are finite; a program needn't handle non-finite values.
Results may differ from the reference program's by a relative error of at most 0.0003.
Values sent between devices are 32-bit elements; how exact they have to be, the bound alone decides.
A program may use at most 128 MiB of HBM per device.

```python
import jax
import jax.numpy as jnp
from jax import lax

TH1 = 32
PH1 = 128
K1 = 4096
K2 = 16384
PB_DEV = 32
HB = 16
B2 = 128
B1 = 512
NLIST = 30
NOFF = 316
TAPS = 4
N_BOX = 4


def draw_interp_index(key, part):
    theta_key, phi_key = jax.random.split(jax.random.fold_in(key, 3), 2)
    rows = jnp.arange(K2, dtype=jnp.int32)[:, None]
    theta_parent = rows // (2 * PH1)
    phi_parent = rows % (2 * PH1)
    theta_centre = theta_parent // 2
    phi_centre = phi_parent // 2
    column = jax.lax.broadcasted_iota(jnp.int32, (K2, TAPS), 1)
    theta_move = jax.random.randint(theta_key, (K2, TAPS), -1, 2)
    theta_move = jnp.where(column == 0, 1 - 2 * (theta_parent % 2), theta_move)
    phi_move = jax.random.randint(phi_key, (K2, TAPS), -2, 3)
    phi_move = jnp.where(column == 1, 2, phi_move)
    theta_child = jnp.clip(theta_centre + theta_move, 0, TH1 - 1)
    phi_child = (phi_centre + phi_move + PH1) % PH1
    return (theta_child * PH1 + phi_child).astype(jnp.int32)


def draw_partners(key, part):
    first_key, second_key = jax.random.split(jax.random.fold_in(key, 7), 2)
    boxes = jnp.arange(B2, dtype=jnp.int32)[:, None]
    distance = jax.random.randint(first_key, (B2, NLIST), 1, HB + 1)
    column = jax.lax.broadcasted_iota(jnp.int32, (B2, NLIST), 1)
    distance = jnp.where(column == 0, HB, distance)
    signs = 2 * jax.random.randint(second_key, (B2, NLIST), 0, 2) - 1
    target = boxes + signs * distance
    outside = (target < 0) | (target >= B2)
    return jnp.where(outside, boxes - signs * distance, target).astype(jnp.int32)


def with_ends(array, own_key, smallest, top_value):
    longest = array.shape.index(max(array.shape))
    spots = []
    for shift in (0, 1):
        where = [jax.random.randint(jax.random.fold_in(own_key, axis), (), 0, length) for axis, length in enumerate(array.shape)]
        where[longest] = (where[longest] + shift) % array.shape[longest]
        spots.append(tuple(where))
    return array.at[spots[0]].set(smallest).at[spots[1]].set(top_value)


def block_scale(key, shape, pieces, smallest, top_value):
    level = 1.0
    for axis_at, parts in pieces:
        heights = jax.random.uniform(jax.random.fold_in(jax.random.fold_in(key, 6), axis_at), (parts,), jnp.float32, smallest / len(pieces), top_value / len(pieces))
        level = level * jnp.repeat(jnp.exp(heights), shape[axis_at] // parts).reshape((-1,) + (1,) * (len(shape) - 1 - axis_at))
    return level


def normal_values(own_key, shape, scale, reach, cuts=(), held_as=jnp.bfloat16):
    result = scale * jax.random.normal(own_key, shape, jnp.float32)
    if cuts:
        result = result * block_scale(own_key, shape, cuts, -0.22, 0.18)
    return jnp.clip(result, -reach, reach).astype(held_as)


def setup_inputs(seed: int = 0) -> dict:
    streams_of = jax.random.split(jax.random.key(seed), 9)
    return {
        "fine_out": normal_values(streams_of[0], (2, B1, K1), 1.0, 6.0, ((1, 4), (2, 8)), jnp.float32),
        "interp_index": draw_interp_index(jax.random.fold_in(streams_of[8], 71), 0),
        "interp_weight": jnp.clip(0.05 + 0.45 * jax.random.uniform(streams_of[2], (K2, TAPS), jnp.float32) ** block_scale(streams_of[2], (K2, TAPS), ((0, 8),), -0.2, 0.2), 0.05, 0.5),
        "child_angle": jnp.clip(jax.random.uniform(streams_of[3], (4, K2), jnp.float32, -3.140625, 3.140625), -3.140625, 3.140625),
        "translator": normal_values(streams_of[4], (2, NOFF, K2), 0.25, 4.0, ((2, 8),), jnp.float32),
        "partners": draw_partners(jax.random.fold_in(streams_of[8], 71), 0),
        "offsets": with_ends(jax.random.randint(streams_of[6], (B2, NLIST), 0, NOFF), jax.random.fold_in(streams_of[6], 1), 0, NOFF - 1).astype(jnp.int32),
        "list_count": with_ends(jax.random.randint(streams_of[7], (B2,), NLIST // 2, NLIST + 1), jax.random.fold_in(streams_of[7], 1), NLIST // 2, NLIST).astype(jnp.int32),
    }


def reference(fine_out, interp_index, interp_weight, child_angle, translator, partners, offsets, list_count):
    cosines = jnp.cos(child_angle)
    sine_part = jnp.sin(child_angle)

    def aggregate(block_number):
        child_rows = lax.dynamic_slice_in_dim(fine_out, block_number * 4 * PB_DEV, 4 * PB_DEV, 1)
        tapped = child_rows[:, :, interp_index]
        interpolated = jnp.sum(tapped * interp_weight, axis=3).reshape(2, PB_DEV, 4, K2)
        real_part = interpolated[0] * cosines - interpolated[1] * sine_part
        imag_part = interpolated[0] * sine_part + interpolated[1] * cosines
        return jnp.stack([jnp.sum(real_part, axis=1), jnp.sum(imag_part, axis=1)])

    coarse_out = lax.map(aggregate, jnp.arange(N_BOX, dtype=jnp.int32))
    coarse_out = jnp.transpose(coarse_out, (1, 0, 2, 3)).reshape(2, B2, K2)

    def incoming(block_number):
        partner_rows = lax.dynamic_slice_in_dim(partners, block_number * PB_DEV, PB_DEV, 0)
        offset_rows = lax.dynamic_slice_in_dim(offsets, block_number * PB_DEV, PB_DEV, 0)
        count_rows = lax.dynamic_slice_in_dim(list_count, block_number * PB_DEV, PB_DEV, 0)

        def add_slot(number, running):
            source = coarse_out[:, partner_rows[:, number]]
            factor = translator[:, offset_rows[:, number]]
            active = (number < count_rows)[:, None]
            real_part = factor[0] * source[0] - factor[1] * source[1]
            imag_part = factor[0] * source[1] + factor[1] * source[0]
            return running + jnp.where(active, jnp.stack([real_part, imag_part]), 0.0)

        parent_in = lax.fori_loop(0, NLIST, add_slot, jnp.zeros((2, PB_DEV, K2), jnp.float32))
        real_part = parent_in[0][:, None, :] * cosines + parent_in[1][:, None, :] * sine_part
        imag_part = parent_in[1][:, None, :] * cosines - parent_in[0][:, None, :] * sine_part
        rotated = jnp.stack([real_part, imag_part]).reshape(2, 4 * PB_DEV, K2)
        spread = jnp.zeros((2, 4 * PB_DEV, K1), jnp.float32)
        for tap_number in range(TAPS):
            spread = spread.at[:, :, interp_index[:, tap_number]].add(rotated * interp_weight[:, tap_number])
        return spread

    fine_in = lax.map(incoming, jnp.arange(N_BOX, dtype=jnp.int32))
    return jnp.transpose(fine_in, (1, 0, 2, 3)).reshape(2, B1, K1)
```

```python
import functools

import jax
import jax.numpy as jnp
from jax import lax
from jax.experimental import pallas as pl
from jax.experimental.pallas import tpu as pltpu
from jax.sharding import PartitionSpec as P

LANES = 128
TAPS = 4
CHILDREN = 4


def split(x):
    hi = x.astype(jnp.bfloat16)
    return hi, (x - hi.astype(jnp.float32)).astype(jnp.bfloat16)


def taps_of(idx_ref, w_ref, first_fine, m):
    width = 4 * LANES
    window = 3 * LANES
    position = lax.broadcasted_iota(jnp.int32, (window, width), 0) + (first_fine + (m - 1) * LANES)
    total = jnp.zeros((window, width), jnp.float32)
    for t in range(TAPS):
        idx = idx_ref[t : t + 1, m * width : (m + 1) * width]
        w = w_ref[t : t + 1, m * width : (m + 1) * width]
        total = total + jnp.where(idx == position, w, 0.0)
    return split(total)


def dot3(a, b, dims):
    ahi, alo = a
    bhi, blo = b
    d = functools.partial(lax.dot_general, dimension_numbers=(dims, ((), ())), preferred_element_type=jnp.float32)
    return d(ahi, bhi) + (d(ahi, blo) + d(alo, bhi))


def kernel(
    partners_in, offsets_in, count_in, fine_in, idx_in, w_in, angle_in, translator, out,
    partners, offsets, count, fine, idx, w, angle, in_sem, low, high, mat_hi, mat_lo, stage, src, swp, trn, p_re, p_im, acc, got_low, got_high, order,
    halo_send, halo_recv, box_send, box_recv, rim_send, rim_recv, trn_sem,
):
    pairs = (
        (fine_in, fine), (idx_in, idx), (w_in, w), (angle_in, angle),
        (partners_in, partners), (offsets_in, offsets), (count_in, count),
    )
    loads = [pltpu.make_async_copy(a, b, in_sem.at[i]) for i, (a, b) in enumerate(pairs)]
    for copy in loads:
        copy.start()
    _, children, cols = fine.shape
    thetas = cols // LANES
    parents = children // CHILDREN
    half = parents // 2
    tiles = angle.shape[1] // LANES
    noff = translator.shape[0]
    nlist = partners.shape[1]
    pitch = src.shape[1]
    width = 4 * LANES
    d, nd = lax.axis_index("dir"), lax.axis_size("dir")
    x, nx = lax.axis_index("box"), lax.axis_size("box")
    has = {"down": d > 0, "up": d < nd - 1, "left": x > 0, "right": x < nx - 1}
    ids = {"down": {"dir": d - 1}, "up": {"dir": d + 1}, "left": {"box": x - 1}, "right": {"box": x + 1}}

    load = pltpu.make_async_copy(translator, trn.at[pl.ds(0, noff)], trn_sem)
    load.start()

    barrier = pltpu.get_barrier_semaphore()
    for side in ids:
        @pl.when(has[side])
        def _(side=side):
            pl.semaphore_signal(barrier, inc=1, device_id=ids[side], device_id_type=MESH)
    pl.semaphore_wait(barrier, sum(jnp.where(here, 1, 0) for here in has.values()))

    def remote(source, target, send, recv, side):
        return pltpu.make_async_remote_copy(
            src_ref=source, dst_ref=target, send_sem=send, recv_sem=recv,
            device_id=ids[side], device_id_type=MESH,
        )

    def when_do(side, copy, act):
        @pl.when(has[side])
        def _():
            getattr(copy, act)()

    to_up = remote(fine.at[:, :, pl.ds(cols - LANES, LANES)], low, halo_send.at[0], halo_recv.at[0], "up")
    to_down = remote(fine.at[:, :, pl.ds(0, LANES)], high, halo_send.at[1], halo_recv.at[1], "down")
    loads[0].wait()
    when_do("up", to_up, "start")
    when_do("down", to_down, "start")

    @pl.when(d == 0)
    def _():
        low[...] = jnp.zeros_like(low)

    @pl.when(d == nd - 1)
    def _():
        high[...] = jnp.zeros_like(high)

    @pl.when(x == 0)
    def _():
        src[:half] = jnp.zeros((half, pitch, LANES), jnp.float32)

    @pl.when(x == nx - 1)
    def _():
        src[half + parents :] = jnp.zeros((half, pitch, LANES), jnp.float32)

    trn[noff] = jnp.zeros((2 * tiles, LANES), jnp.float32)
    for copy in loads[1:]:
        copy.wait()
    first = d * cols
    cos = jnp.cos(angle[...])
    sin = jnp.sin(angle[...])
    for m in range(thetas):
        mat_hi[m], mat_lo[m] = taps_of(idx, w, first, m)

    def tile(k):
        if k < 0:
            return low[...].reshape(2 * children, LANES)
        if k == thetas:
            return high[...].reshape(2 * children, LANES)
        return fine[:, :, k * LANES : (k + 1) * LANES].reshape(2 * children, LANES)

    src2 = src.reshape(2 * parents * pitch, LANES)

    def chunk(m, side):
        rows = pl.ds(2 * 4 * m, 8)
        if side == "left":
            source, target, n = half, half + parents, 0
        else:
            source, target, n = parents, 0, 1
        return remote(
            src.at[pl.ds(source, half), rows, :], src.at[pl.ds(target, half), rows, :],
            box_send.at[n, m], box_recv.at[n, m], side,
        )

    def aggregate(m):
        a = split(jnp.concatenate([tile(m - 1), tile(m), tile(m + 1)], axis=1))
        y = dot3(a, (mat_hi[m], mat_lo[m]), ((1,), (0,)))
        for i in range(4):
            stage[i] = y[:, i * LANES : (i + 1) * LANES]
        for i in range(4):
            k = 4 * m + i
            re = im = None
            for c in range(CHILDREN):
                xr = stage[i, pl.ds(c, parents, stride=CHILDREN), :]
                xi = stage[i, pl.ds(children + c, parents, stride=CHILDREN), :]
                cc = cos[c : c + 1, k * LANES : (k + 1) * LANES]
                sc = sin[c : c + 1, k * LANES : (k + 1) * LANES]
                r, j = xr * cc - xi * sc, xr * sc + xi * cc
                re, im = (r, j) if c == 0 else (re + r, im + j)
            src2[pl.ds(half * pitch + 2 * k, parents, stride=pitch), :] = re
            src2[pl.ds(half * pitch + 2 * k + 1, parents, stride=pitch), :] = im
        for side in ("left", "right"):
            when_do(side, chunk(m, side), "start")

    for m in range(1, thetas - 1):
        aggregate(m)
    when_do("down", to_up, "wait_recv")
    when_do("up", to_down, "wait_recv")
    for m in sorted({0, thetas - 1}):
        aggregate(m)
    when_do("up", to_up, "wait_send")
    when_do("down", to_down, "wait_send")
    even = lax.broadcasted_iota(jnp.int32, (2 * tiles, LANES), 0) % 2 == 0

    def swap(p, carry):
        v = src[p, : 2 * tiles, :]
        swp[p] = jnp.where(even, pltpu.roll(v, 2 * tiles - 1, 0), pltpu.roll(v, 1, 0))
        return carry

    lax.fori_loop(half, half + parents, swap, 0, unroll=4)
    for m in range(thetas):
        when_do("right", chunk(m, "left"), "wait_recv")
        when_do("left", chunk(m, "right"), "wait_recv")
    lax.fori_loop(0, half, swap, 0, unroll=4)
    lax.fori_loop(half + parents, 2 * parents, swap, 0, unroll=4)
    load.wait()
    base = x * parents - half

    def box(b, carry):
        used = count[b]
        one = two = None
        for s in range(nlist):
            o = jnp.where(s < used, offsets[b, s], noff)
            p = jnp.maximum(partners[b, s] - base, 0)
            t = trn[o]
            u, v = t * src[p, : 2 * tiles, :], t * swp[p]
            one, two = (u, v) if s == 0 else (one + u, two + v)
        p_re[b, : 2 * tiles, :] = one
        p_im[b, : 2 * tiles, :] = two
        return carry

    lax.fori_loop(0, parents, box, 0)
    r2 = p_re.reshape(parents * pitch, LANES)
    i2 = p_im.reshape(parents * pitch, LANES)

    def spread(m):
        def part(ref, k, c):
            return ref[pl.ds(2 * k + c, parents, stride=pitch), :]

        pr = jnp.concatenate([part(r2, 4 * m + i, 0) - part(r2, 4 * m + i, 1) for i in range(4)], axis=1)
        pi = jnp.concatenate([part(i2, 4 * m + i, 0) + part(i2, 4 * m + i, 1) for i in range(4)], axis=1)
        res, ims = [], []
        for c in range(CHILDREN):
            cc = cos[c : c + 1, m * width : (m + 1) * width]
            sc = sin[c : c + 1, m * width : (m + 1) * width]
            res.append(pr * cc + pi * sc)
            ims.append(pi * cc - pr * sc)
        rot = split(jnp.concatenate(res + ims, axis=0))
        y = dot3(rot, (mat_hi[m], mat_lo[m]), ((1,), (1,)))
        for i in range(3):
            v = y[:, i * LANES : (i + 1) * LANES]
            if m + i in seen:
                acc[m + i] += v
            else:
                acc[m + i] = v
                seen.add(m + i)

    seen = set()
    rim_down = remote(acc.at[0], got_high, rim_send.at[0], rim_recv.at[0], "down")
    rim_up = remote(acc.at[thetas + 1], got_low, rim_send.at[1], rim_recv.at[1], "up")
    spread(0)
    when_do("down", rim_down, "start")
    if thetas > 1:
        spread(thetas - 1)
    when_do("up", rim_up, "start")

    @pl.when(d == 0)
    def _():
        got_low[...] = jnp.zeros_like(got_low)

    @pl.when(d == nd - 1)
    def _():
        got_high[...] = jnp.zeros_like(got_high)

    for m in range(1, thetas - 1):
        spread(m)
    when_do("up", rim_down, "wait_recv")
    when_do("down", rim_up, "wait_recv")
    for k in range(1, thetas + 1):
        for comp in range(2):
            for c in range(CHILDREN):
                rows = pl.ds((comp * CHILDREN + c) * parents, parents)
                v = acc[k, rows, :]
                if k == 1:
                    v = v + got_low[rows, :]
                if k == thetas:
                    v = v + got_high[rows, :]
                order[k - 1, comp, pl.ds(c, parents, stride=CHILDREN), :] = v
        out[:, :, (k - 1) * LANES : k * LANES] = order[k - 1]
    when_do("down", rim_down, "wait_send")
    when_do("up", rim_up, "wait_send")
    for m in range(thetas):
        for side in ("left", "right"):
            when_do(side, chunk(m, side), "wait_send")


VMEM = pl.BlockSpec(memory_space=pltpu.VMEM)
HBM = pl.BlockSpec(memory_space=pltpu.HBM)
MESH = pl.DeviceIdType.MESH


def shards(fine_out, interp_index, interp_weight, child_angle, translator, partners, offsets, list_count):
    _, children, cols = fine_out.shape
    parents = partners.shape[0]
    samples = child_angle.shape[1]
    noff = translator.shape[1]
    tiles = samples // LANES
    thetas = cols // LANES
    pitch = 2 * tiles + 8
    f32, bf16 = jnp.float32, jnp.bfloat16
    ordered = translator.reshape(2, noff, tiles, LANES).transpose(1, 2, 0, 3).reshape(noff, 2 * tiles, LANES)
    dma = pltpu.SemaphoreType.DMA
    return pl.pallas_call(
        kernel,
        out_shape=jax.ShapeDtypeStruct((2, children, cols), f32),
        in_specs=[HBM] * 8,
        out_specs=VMEM,
        scratch_shapes=[
            pltpu.SMEM(partners.shape, jnp.int32),
            pltpu.SMEM(offsets.shape, jnp.int32),
            pltpu.SMEM(list_count.shape, jnp.int32),
            pltpu.VMEM(fine_out.shape, f32),
            pltpu.VMEM((TAPS, samples), jnp.int32),
            pltpu.VMEM((TAPS, samples), f32),
            pltpu.VMEM(child_angle.shape, f32),
            dma((7,)),
            pltpu.VMEM((2, children, LANES), f32),
            pltpu.VMEM((2, children, LANES), f32),
            pltpu.VMEM((thetas, 3 * LANES, 4 * LANES), bf16),
            pltpu.VMEM((thetas, 3 * LANES, 4 * LANES), bf16),
            pltpu.VMEM((4, 2 * children, LANES), f32),
            pltpu.VMEM((2 * parents, pitch, LANES), f32),
            pltpu.VMEM((2 * parents, 2 * tiles, LANES), f32),
            pltpu.VMEM((noff + 1, 2 * tiles, LANES), f32),
            pltpu.VMEM((parents, pitch, LANES), f32),
            pltpu.VMEM((parents, pitch, LANES), f32),
            pltpu.VMEM((thetas + 2, 2 * children, LANES), f32),
            pltpu.VMEM((2 * children, LANES), f32),
            pltpu.VMEM((2 * children, LANES), f32),
            pltpu.VMEM((thetas, 2, children, LANES), f32),
            dma((2,)), dma((2,)), dma((2, thetas)), dma((2, thetas)), dma((2,)), dma((2,)), dma,
        ],
        compiler_params=pltpu.CompilerParams(
            vmem_limit_bytes=41943040, collective_id=0, has_side_effects=True
        ),
    )(*(pltpu.with_memory_space_constraint(v, pltpu.HBM) for v in (partners, offsets, list_count, fine_out, interp_index.T, interp_weight.T, child_angle, ordered)))


def solution(mesh):
    placed = (
        P(None, "box", "dir"),
        P("dir", None),
        P("dir", None),
        P(None, "dir"),
        P(None, None, "dir"),
        P("box", None),
        P("box", None),
        P("box"),
    )
    return jax.shard_map(
        shards, mesh=mesh, in_specs=placed, out_specs=P(None, "box", "dir"), check_vma=False
    )
```

```python
import functools

import jax
import jax.numpy as jnp
from jax import lax
from jax.experimental import pallas as pl
from jax.experimental.pallas import tpu as pltpu
from jax.sharding import PartitionSpec as P

LANES = 128
TAPS = 4
CHILDREN = 4
PITCH = 24


def split(x):
    hi = x.astype(jnp.bfloat16)
    return hi, (x - hi.astype(jnp.float32)).astype(jnp.bfloat16)


def dot(a, b, dims):
    return lax.dot_general(a, b, dimension_numbers=(dims, ((), ())), preferred_element_type=jnp.float32)


def kernel(
    partners_in, offsets_in, count_in, fine_in, idx_in, w_in, angle_in, translator, out,
    count, rows_p, rows_o, slot_p, slot_o, fine, idx, w, angle, fine_sem, in_sem, slot_sem, low, high,
    mat_hi, mat_lo, srcs, trn, par, rot_hi, rot_lo, acc, got_low, got_high, order,
    halo_send, halo_recv, box_send, box_recv, rim_send, rim_recv, trn_sem,
):
    thetas, _, children, _ = fine.shape
    parents = children // CHILDREN
    half = parents // 2
    tiles = angle.shape[1] // LANES
    noff = translator.shape[0] // thetas
    boxed = [src.reshape(2 * parents, PITCH, LANES) for src in srcs]
    flat = [src.reshape(2 * parents * PITCH, LANES) for src in srcs]
    nlist = rows_p.shape[1]
    width = 4 * LANES
    last = thetas - 1
    edges = sorted({0, last})
    inner = tuple(range(1, last))
    d, nd = lax.axis_index("dir"), lax.axis_size("dir")
    x, nx = lax.axis_index("box"), lax.axis_size("box")
    has = {"down": d > 0, "up": d < nd - 1, "left": x > 0, "right": x < nx - 1}
    ids = {"down": {"dir": d - 1}, "up": {"dir": d + 1}, "left": {"box": x - 1}, "right": {"box": x + 1}}

    fine_loads = {
        k: pltpu.make_async_copy(fine_in.at[:, :, pl.ds(k * LANES, LANES)], fine.at[k], fine_sem.at[k])
        for k in (*edges, *inner)
    }
    pairs = ((idx_in, idx), (w_in, w), (angle_in, angle), (partners_in, rows_p), (offsets_in, rows_o), (count_in, count))
    loads = [pltpu.make_async_copy(a, b, in_sem.at[i]) for i, (a, b) in enumerate(pairs)]
    for copy in (*fine_loads.values(), *loads):
        copy.start()
    load = pltpu.make_async_copy(translator, trn.at[pl.ds(0, noff * thetas)], trn_sem)
    load.start()

    barrier = pltpu.get_barrier_semaphore()
    for side in ids:
        @pl.when(has[side])
        def _(side=side):
            pl.semaphore_signal(barrier, inc=1, device_id=ids[side], device_id_type=MESH)
    pl.semaphore_wait(barrier, sum(jnp.where(here, 1, 0) for here in has.values()))

    def remote(source, target, send, recv, side):
        return pltpu.make_async_remote_copy(
            src_ref=source, dst_ref=target, send_sem=send, recv_sem=recv,
            device_id=ids[side], device_id_type=MESH,
        )

    def when_do(side, copy, act):
        @pl.when(has[side])
        def _():
            getattr(copy, act)()

    to_up = remote(fine.at[last], low, halo_send.at[0], halo_recv.at[0], "up")
    to_down = remote(fine.at[0], high, halo_send.at[1], halo_recv.at[1], "down")
    for k in edges:
        fine_loads[k].wait()
    when_do("up", to_up, "start")
    when_do("down", to_down, "start")

    @pl.when(d == 0)
    def _():
        low[...] = jnp.zeros_like(low)

    @pl.when(d == nd - 1)
    def _():
        high[...] = jnp.zeros_like(high)

    @pl.when(x == 0)
    def _():
        for src in boxed:
            src[:half] = jnp.zeros((half, PITCH, LANES), jnp.float32)

    @pl.when(x == nx - 1)
    def _():
        for src in boxed:
            src[half + parents :] = jnp.zeros((half, PITCH, LANES), jnp.float32)

    trn[noff * thetas :] = jnp.zeros((thetas, 8, LANES), jnp.float32)
    for copy in loads:
        copy.wait()
    for k in inner:
        fine_loads[k].wait()
    first = d * thetas * LANES
    cos = jnp.cos(angle[...])
    sin = jnp.sin(angle[...])

    def phase(c, k, n):
        return cos[c : c + 1, k * LANES : (k + n) * LANES], sin[c : c + 1, k * LANES : (k + n) * LANES]

    def taps(m):
        position = lax.broadcasted_iota(jnp.int32, (3 * LANES, width), 0) + (first + (m - 1) * LANES)
        total = jnp.zeros((3 * LANES, width), jnp.float32)
        for t in range(TAPS):
            at = idx[t : t + 1, m * width : (m + 1) * width]
            total = total + jnp.where(at == position, w[t : t + 1, m * width : (m + 1) * width], 0.0)
        mat_hi[m], mat_lo[m] = split(total)

    def tile(k):
        ref = low if k < 0 else high if k == thetas else fine.at[k]
        return split(jnp.concatenate(
            [ref[comp, pl.ds(c, parents, stride=CHILDREN), :] for comp in range(2) for c in range(CHILDREN)], axis=0
        ))

    par2 = par.reshape(thetas * parents * PITCH, LANES)

    def gather(m, ks, fresh):
        a = [tile(k) for k in ks]
        hi, lo = [v[0] for v in a], [v[1] for v in a]
        cut = [pl.ds((k - m + 1) * LANES, LANES) for k in ks]
        bhi, blo = [mat_hi[m, s, :] for s in cut], [mat_lo[m, s, :] for s in cut]
        y = dot(jnp.concatenate(hi + lo + hi, axis=1), jnp.concatenate(bhi + bhi + blo, axis=0), ((1,), (0,)))
        for i in range(4):
            re = im = None
            for c in range(CHILDREN):
                xr = y[c * parents : (c + 1) * parents, i * LANES : (i + 1) * LANES]
                xi = y[children + c * parents : children + (c + 1) * parents, i * LANES : (i + 1) * LANES]
                cc, sc = phase(c, 4 * m + i, 1)
                r, j = xr * cc - xi * sc, xr * sc + xi * cc
                re, im = (r, j) if c == 0 else (re + r, im + j)
            src, at = flat[m], half * PITCH + 2 * i

            def own(row):
                return pl.ds(at + row, parents, stride=PITCH)

            if not fresh:
                re, im = re + src[own(0), :], im + src[own(1), :]
            src[own(0), :] = re
            src[own(1), :] = im
            src[own(8), :] = im
            src[own(9), :] = re

    def chunk(m, side):
        if side == "left":
            source, target, n = half, half + parents, 0
        else:
            source, target, n = parents, 0, 1
        rows = pl.ds(0, 8)
        return remote(
            boxed[m].at[pl.ds(source, half), rows, :], boxed[m].at[pl.ds(target, half), rows, :],
            box_send.at[n, m], box_recv.at[n, m], side,
        )

    def boxes_out(m):
        for side in ("left", "right"):
            when_do(side, chunk(m, side), "start")

    even = lax.broadcasted_iota(jnp.int32, (8, LANES), 0) % 2 == 0

    def boxes_in(m):
        when_do("right", chunk(m, "left"), "wait_recv")
        when_do("left", chunk(m, "right"), "wait_recv")
        for p in (*range(half), *range(half + parents, 2 * parents)):
            v = boxed[m][p, :8, :]
            boxed[m][p, 8:16, :] = jnp.where(even, pltpu.roll(v, 7, 0), pltpu.roll(v, 1, 0))

    def translate(ms):
        def box(b, carry):
            one, two = {}, {}
            for s in range(nlist):
                o, p = slot_o[b, s], slot_p[b, s]
                for m in ms:
                    t = trn[o + m]
                    u, v = t * srcs[m][p], t * srcs[m][p + 1]
                    key = m, s % 2
                    one[key], two[key] = (u, v) if s < 2 else (one[key] + u, two[key] + v)
            for m in ms:
                par[m, b, 0:8, :] = sum(one[m, n] for n in range(min(2, nlist)))
                par[m, b, 8:16, :] = sum(two[m, n] for n in range(min(2, nlist)))
            return carry

        lax.fori_loop(0, parents, box, 0)

    seen = set()

    def put(k, v):
        if k in seen:
            acc[k] += v
        else:
            acc[k] = v
            seen.add(k)

    def rotate(m):
        def part(row):
            return par2[pl.ds(m * parents * PITCH + row, parents, stride=PITCH), :]

        pr = jnp.concatenate([part(2 * i) - part(2 * i + 1) for i in range(4)], axis=1)
        pi = jnp.concatenate([part(8 + 2 * i) + part(9 + 2 * i) for i in range(4)], axis=1)
        for c in range(CHILDREN):
            cc, sc = phase(c, 4 * m, 4)
            for comp, v in enumerate((pr * cc + pi * sc, pi * cc - pr * sc)):
                rows = pl.ds((comp * CHILDREN + c) * parents, parents)
                rot_hi[rows, :], rot_lo[rows, :] = split(v)

    def spread(m, i):
        bhi, blo = mat_hi[m, pl.ds(i * LANES, LANES), :], mat_lo[m, pl.ds(i * LANES, LANES), :]
        y = dot(rot_hi[...], jnp.concatenate([bhi, blo], axis=0), ((1,), (1,)))
        put(m + i, y[:, :LANES] + (y[:, LANES:] + dot(rot_lo[...], bhi, ((1,), (1,)))))

    def spread2(m, i):
        rows = pl.ds(i * LANES, 2 * LANES)
        bhi, blo = mat_hi[m, rows, :], mat_lo[m, rows, :]
        y = dot(rot_hi[...], bhi, ((1,), (1,))) + (
            dot(rot_hi[...], blo, ((1,), (1,))) + dot(rot_lo[...], bhi, ((1,), (1,)))
        )
        put(m + i, y[:, :LANES])
        put(m + i + 1, y[:, LANES:])

    base = x * parents - half

    def tables():
        shape = (parents, nlist)
        row, slot = lax.broadcasted_iota(jnp.int32, shape, 0), lax.broadcasted_iota(jnp.int32, shape, 1)
        used = jnp.zeros(shape, jnp.int32)
        for b in range(parents):
            used = jnp.where(row == b, count[b], used)
        rows_o[...] = jnp.where(slot < used, rows_o[...], noff) * thetas
        rows_p[...] = jnp.maximum(rows_p[...] - base, 0) * (PITCH // 8)

    slots = [
        pltpu.make_async_copy(rows_p, slot_p, slot_sem.at[0]),
        pltpu.make_async_copy(rows_o, slot_o, slot_sem.at[1]),
    ]
    rim_down = remote(acc.at[0], got_high, rim_send.at[0], rim_recv.at[0], "down")
    rim_up = remote(acc.at[thetas + 1], got_low, rim_send.at[1], rim_recv.at[1], "up")

    with jax.named_scope("k_tables"):
        tables()
    for copy in slots:
        copy.start()
    with jax.named_scope("k_inner"):
        for m in inner:
            taps(m)
            gather(m, (m - 1, m, m + 1), True)
            boxes_out(m)
    with jax.named_scope("k_local"):
        for m in edges:
            taps(m)
            gather(m, [k for k in (m - 1, m, m + 1) if 0 <= k < thetas], True)
    with jax.named_scope("k_lowwait"):
        when_do("down", to_up, "wait_recv")
    if thetas == 1:
        when_do("up", to_down, "wait_recv")
    with jax.named_scope("k_halo0"):
        gather(0, (-1, 1) if thetas == 1 else (-1,), False)
        boxes_out(0)
    for copy in slots:
        copy.wait()
    with jax.named_scope("k_trnwait"):
        load.wait()
    if inner:
        with jax.named_scope("k_boxin12"):
            for m in inner:
                boxes_in(m)
        with jax.named_scope("k_tr12"):
            translate(inner)
    with jax.named_scope("k_boxin0"):
        boxes_in(0)
    with jax.named_scope("k_tr0"):
        translate((0,))
    if thetas > 1:
        with jax.named_scope("k_highwait"):
            when_do("up", to_down, "wait_recv")
        with jax.named_scope("k_halo3"):
            gather(last, (thetas,), False)
            boxes_out(last)
    with jax.named_scope("k_rim0"):
        rotate(0)
        spread(0, 0)
        when_do("down", rim_down, "start")
    if thetas == 1:
        spread(0, 2)
        when_do("up", rim_up, "start")
        spread(0, 1)
    else:
        with jax.named_scope("k_rest0"):
            spread2(0, 1)
        with jax.named_scope("k_spread12"):
            for m in inner:
                rotate(m)
                spread2(m, 0)
                spread(m, 2)
        with jax.named_scope("k_boxin3"):
            boxes_in(last)
        with jax.named_scope("k_tr3"):
            translate((last,))
        with jax.named_scope("k_rim3"):
            rotate(last)
            spread(last, 2)
            when_do("up", rim_up, "start")
        with jax.named_scope("k_rest3"):
            spread2(last, 0)

    @pl.when(d == 0)
    def _():
        got_low[...] = jnp.zeros_like(got_low)

    @pl.when(d == nd - 1)
    def _():
        got_high[...] = jnp.zeros_like(got_high)

    def result(k):
        for comp in range(2):
            for c in range(CHILDREN):
                rows = pl.ds((comp * CHILDREN + c) * parents, parents)
                v = acc[k, rows, :]
                if k == 1:
                    v = v + got_low[rows, :]
                if k == thetas:
                    v = v + got_high[rows, :]
                order[k - 1, comp, pl.ds(c, parents, stride=CHILDREN), :] = v
        out[:, :, (k - 1) * LANES : k * LANES] = order[k - 1]

    for k in range(2, thetas):
        result(k)
    with jax.named_scope("k_rimwait"):
        when_do("up", rim_down, "wait_recv")
        if thetas > 1:
            result(thetas)
    with jax.named_scope("k_rimwait2"):
        when_do("down", rim_up, "wait_recv")
    with jax.named_scope("k_end"):
        result(1)
    when_do("up", to_up, "wait_send")
    when_do("down", to_down, "wait_send")
    when_do("down", rim_down, "wait_send")
    when_do("up", rim_up, "wait_send")
    for m in range(thetas):
        for side in ("left", "right"):
            when_do(side, chunk(m, side), "wait_send")


VMEM = pl.BlockSpec(memory_space=pltpu.VMEM)
HBM = pl.BlockSpec(memory_space=pltpu.HBM)
MESH = pl.DeviceIdType.MESH


def shards(fine_out, interp_index, interp_weight, child_angle, translator, partners, offsets, list_count):
    _, children, cols = fine_out.shape
    parents = partners.shape[0]
    samples = child_angle.shape[1]
    noff = translator.shape[1]
    tiles = samples // LANES
    thetas = cols // LANES
    f32, bf16 = jnp.float32, jnp.bfloat16
    ordered = translator.reshape(2, noff, tiles, LANES).transpose(1, 2, 0, 3).reshape(noff * thetas, 8, LANES)
    dma = pltpu.SemaphoreType.DMA
    operands = (partners, offsets, list_count, fine_out, interp_index.T, interp_weight.T, child_angle, ordered)
    return pl.pallas_call(
        kernel,
        out_shape=jax.ShapeDtypeStruct((2, children, cols), f32),
        in_specs=[HBM] * 8,
        out_specs=VMEM,
        scratch_shapes=[
            pltpu.SMEM(list_count.shape, jnp.int32),
            pltpu.VMEM(partners.shape, jnp.int32),
            pltpu.VMEM(offsets.shape, jnp.int32),
            pltpu.SMEM(partners.shape, jnp.int32),
            pltpu.SMEM(offsets.shape, jnp.int32),
            pltpu.VMEM((thetas, 2, children, LANES), f32),
            pltpu.VMEM((TAPS, samples), jnp.int32),
            pltpu.VMEM((TAPS, samples), f32),
            pltpu.VMEM(child_angle.shape, f32),
            dma((thetas,)),
            dma((6,)),
            dma((2,)),
            pltpu.VMEM((2, children, LANES), f32),
            pltpu.VMEM((2, children, LANES), f32),
            pltpu.VMEM((thetas, 3 * LANES, 4 * LANES), bf16),
            pltpu.VMEM((thetas, 3 * LANES, 4 * LANES), bf16),
            [pltpu.VMEM((2 * parents * PITCH // 8, 8, LANES), f32) for _ in range(thetas)],
            pltpu.VMEM(((noff + 1) * thetas, 8, LANES), f32),
            pltpu.VMEM((thetas, parents, PITCH, LANES), f32),
            pltpu.VMEM((2 * children, 4 * LANES), bf16),
            pltpu.VMEM((2 * children, 4 * LANES), bf16),
            pltpu.VMEM((thetas + 2, 2 * children, LANES), f32),
            pltpu.VMEM((2 * children, LANES), f32),
            pltpu.VMEM((2 * children, LANES), f32),
            pltpu.VMEM((thetas, 2, children, LANES), f32),
            dma((2,)), dma((2,)), dma((2, thetas)), dma((2, thetas)), dma((2,)), dma((2,)), dma,
        ],
        compiler_params=pltpu.CompilerParams(
            vmem_limit_bytes=40 * 1024 * 1024, collective_id=0, has_side_effects=True
        ),
    )(*(pltpu.with_memory_space_constraint(v, pltpu.HBM) for v in operands))


def solution(mesh):
    placed = (
        P(None, "box", "dir"),
        P("dir", None),
        P("dir", None),
        P(None, "dir"),
        P(None, None, "dir"),
        P("box", None),
        P("box", None),
        P("box"),
    )
    return jax.shard_map(
        shards, mesh=mesh, in_specs=placed, out_specs=P(None, "box", "dir"), check_vma=False
    )
```

```python
import functools

import jax
import jax.numpy as jnp
from jax import lax
from jax.experimental import pallas as pl
from jax.experimental.pallas import tpu as pltpu
from jax.sharding import PartitionSpec as P

LANES = 128
TAPS = 4
CHILDREN = 4


def pitch(rows):
    return 16 * rows + 8


def split(x):
    hi = x.astype(jnp.bfloat16)
    return hi, (x - hi.astype(jnp.float32)).astype(jnp.bfloat16)


def dot(a, b, dims):
    return lax.dot_general(a, b, dimension_numbers=(dims, ((), ())), preferred_element_type=jnp.float32)


def kernel(
    partners_in, offsets_in, count_in, fine_in, idx_in, w_in, angle_in, translator, out,
    count, rows_p, rows_o, slot_p, slot_i, slot_o, fine, idx, w, angle, cos, sin, fine_sem, in_sem, slot_sem, halo,
    mat_hi, mat_lo, srcs, trn, pre, par, rot_hi, rot_lo, acc, rims, got, order,
    halo_send, halo_recv, box_send, box_recv, rim_send, rim_recv, trn_sem,
):
    thetas, _, children, _ = fine.shape
    parents = children // CHILDREN
    half = parents // 2
    tiles = angle.shape[1] // LANES
    noff = translator.shape[0] // thetas
    nlist = rows_p.shape[1]
    width = 4 * LANES
    last = thetas - 1
    inner = tuple(range(1, last))
    roles = (0, 1) if thetas > 1 else (0,)
    d, nd = lax.axis_index("dir"), lax.axis_size("dir")
    x, nx = lax.axis_index("box"), lax.axis_size("box")
    has = {"down": d > 0, "up": d < nd - 1, "left": x > 0, "right": x < nx - 1}
    ids = {"down": {"dir": d - 1}, "up": {"dir": d + 1}, "left": {"box": x - 1}, "right": {"box": x + 1}}
    is_even = d % 2 == 0
    top = jnp.where(is_even, 0, 1)
    ends = (top, 1 - top)

    fine_loads = {
        k: pltpu.make_async_copy(fine_in.at[:, :, pl.ds(k * LANES, LANES)], fine.at[k], fine_sem.at[k])
        for k in (*sorted({0, last}), *inner)
    }
    pairs = ((idx_in, idx), (w_in, w), (angle_in, angle), (partners_in, rows_p), (offsets_in, rows_o), (count_in, count))
    loads = [pltpu.make_async_copy(a, b, in_sem.at[i]) for i, (a, b) in enumerate(pairs)]
    for copy in (*fine_loads.values(), *loads):
        copy.start()
    load = pltpu.make_async_copy(translator, trn.at[pl.ds(0, noff * thetas)], trn_sem)
    load.start()

    barrier = pltpu.get_barrier_semaphore()
    for side in ids:
        @pl.when(has[side])
        def _(side=side):
            pl.semaphore_signal(barrier, inc=1, device_id=ids[side], device_id_type=MESH)
    pl.semaphore_wait(barrier, sum(jnp.where(here, 1, 0) for here in has.values()))

    def remote(source, target, send, recv, side):
        return pltpu.make_async_remote_copy(
            src_ref=source, dst_ref=target, send_sem=send, recv_sem=recv,
            device_id=ids[side], device_id_type=MESH,
        )

    def when_do(side, copy, act, also=None):
        @pl.when(has[side] if also is None else jnp.logical_and(has[side], also))
        def _():
            getattr(copy, act)()

    to_up = remote(fine.at[last], halo.at[0], halo_send.at[0], halo_recv.at[0], "up")
    to_down = remote(fine.at[0], halo.at[1], halo_send.at[1], halo_recv.at[1], "down")
    for k in sorted({0, last}):
        fine_loads[k].wait()
    when_do("up", to_up, "start")
    when_do("down", to_down, "start")

    @pl.when(d == 0)
    def _():
        halo[0] = jnp.zeros(halo.shape[1:], jnp.float32)

    @pl.when(d == nd - 1)
    def _():
        halo[1] = jnp.zeros(halo.shape[1:], jnp.float32)

    groups = [[m] for m in roles] + ([list(inner)] if inner else [])
    boxed = [src.reshape(2 * parents, pitch(len(g)), LANES) for src, g in zip(srcs, groups)]
    flat = [src.reshape(2 * parents * pitch(len(g)), LANES) for src, g in zip(srcs, groups)]

    @pl.when(x == 0)
    def _():
        for src in boxed:
            src[:half] = jnp.zeros((half, src.shape[1], LANES), jnp.float32)

    @pl.when(x == nx - 1)
    def _():
        for src in boxed:
            src[half + parents :] = jnp.zeros((half, src.shape[1], LANES), jnp.float32)

    trn[noff * thetas :] = jnp.zeros((thetas, 8, LANES), jnp.float32)
    for copy in loads:
        copy.wait()
    for k in inner:
        fine_loads[k].wait()
    first = d * thetas * LANES
    for m in range(thetas):
        cos[m] = jnp.cos(angle[:, m * width : (m + 1) * width])
        sin[m] = jnp.sin(angle[:, m * width : (m + 1) * width])

    def taps(m):
        position = lax.broadcasted_iota(jnp.int32, (3 * LANES, width), 0) + (first + (m - 1) * LANES)
        total = jnp.zeros((3 * LANES, width), jnp.float32)
        for t in range(TAPS):
            at = idx[t : t + 1, m * width : (m + 1) * width]
            total = total + jnp.where(at == position, w[t : t + 1, m * width : (m + 1) * width], 0.0)
        mat_hi[m], mat_lo[m] = split(total)

    def tile(ref, k):
        return split(jnp.concatenate(
            [ref[k, comp, pl.ds(c, parents, stride=CHILDREN), :] for comp in range(2) for c in range(CHILDREN)], axis=0
        ))

    def gather(m, tiles, start, group, place, fresh):
        hi, lo = [v[0] for v in tiles], [v[1] for v in tiles]
        cut = pl.ds(start * LANES, len(tiles) * LANES)
        bhi, blo = mat_hi[m, cut, :], mat_lo[m, cut, :]
        y = dot(jnp.concatenate(hi + lo + hi, axis=1), jnp.concatenate([bhi, bhi, blo], axis=0), ((1,), (0,)))
        src, step = flat[group], boxed[group].shape[1]
        for i in range(4):
            re = im = None
            cut = pl.ds(i * LANES, LANES)
            for c in range(CHILDREN):
                xr = y[c * parents : (c + 1) * parents, i * LANES : (i + 1) * LANES]
                xi = y[children + c * parents : children + (c + 1) * parents, i * LANES : (i + 1) * LANES]
                cc, sc = cos[m, pl.ds(c, 1), cut], sin[m, pl.ds(c, 1), cut]
                r, j = xr * cc - xi * sc, xr * sc + xi * cc
                re, im = (r, j) if c == 0 else (re + r, im + j)

            def own(row):
                return pl.ds(half * step + 16 * place + 2 * i + row, parents, stride=step)

            if not fresh:
                re, im = re + src[own(0), :], im + src[own(1), :]
            src[own(0), :] = re
            src[own(1), :] = im
            src[own(8), :] = im
            src[own(9), :] = re

    def chunk(group, place, side):
        if side == "left":
            source, target, n = half, half + parents, 0
        else:
            source, target, n = parents, 0, 1
        rows = pl.ds(16 * place, 8)
        sem = n, groups[group][place]
        if group < len(roles):
            sem = n, group * last
        return remote(
            boxed[group].at[pl.ds(source, half), rows, :], boxed[group].at[pl.ds(target, half), rows, :],
            box_send.at[sem], box_recv.at[sem], side,
        )

    def boxes_out(group, place):
        for side in ("left", "right"):
            when_do(side, chunk(group, place, side), "start")

    even = lax.broadcasted_iota(jnp.int32, (8, LANES), 0) % 2 == 0

    def boxes_in(group, place):
        when_do("right", chunk(group, place, "left"), "wait_recv")
        when_do("left", chunk(group, place, "right"), "wait_recv")
        src = boxed[group]
        for p in (*range(half), *range(half + parents, 2 * parents)):
            v = src[p, 16 * place : 16 * place + 8, :]
            src[p, 16 * place + 8 : 16 * place + 16, :] = jnp.where(even, pltpu.roll(v, 7, 0), pltpu.roll(v, 1, 0))

    def sums(slots, n):
        one, two = {}, {}
        for s, (t, u, v) in enumerate(slots):
            u, v = t * u, t * v
            one[s % n], two[s % n] = (u, v) if s < n else (one[s % n] + u, two[s % n] + v)
        n = min(n, len(one))
        return sum(one[k] for k in range(n)), sum(two[k] for k in range(n))

    def prepare():
        src = srcs[-1]

        def box(b, carry):
            made = {m: [] for m in inner}
            for s in range(nlist):
                o = slot_o[b, s]
                for role in roles:
                    pre[role, b * nlist + s] = trn[o + role * last]
                if inner:
                    p = slot_i[b, s]
                    for place, m in enumerate(inner):
                        made[m].append((trn[o + m], src[p + 2 * place], src[p + 2 * place + 1]))
            for m in inner:
                par[m, b, 0:8, :], par[m, b, 8:16, :] = sums(made[m], 1)
            return carry

        lax.fori_loop(0, parents, box, 0)

    def translate(role):
        src = srcs[role]
        m = ends[role] if thetas > 1 else 0

        for b in range(parents):
            made = []
            for s in range(nlist):
                p = slot_p[b, s]
                made.append((pre[m, b * nlist + s], src[p], src[p + 1]))
            par[role * last, b, 0:8, :], par[role * last, b, 8:16, :] = sums(made, 2)

    par2 = par.reshape(thetas * parents * pitch(1), LANES)

    def rotate(m, slot):
        def part(row):
            return par2[pl.ds(slot * parents * pitch(1) + row, parents, stride=pitch(1)), :]

        pr = jnp.concatenate([part(2 * i) - part(2 * i + 1) for i in range(4)], axis=1)
        pi = jnp.concatenate([part(8 + 2 * i) + part(9 + 2 * i) for i in range(4)], axis=1)
        for c in range(CHILDREN):
            cc, sc = cos[m, pl.ds(c, 1), :], sin[m, pl.ds(c, 1), :]
            for comp, v in enumerate((pr * cc + pi * sc, pi * cc - pr * sc)):
                rows = pl.ds((comp * CHILDREN + c) * parents, parents)
                rot_hi[slot, rows, :], rot_lo[slot, rows, :] = split(v)

    def spread(m, slot, i):
        cut = pl.ds(i * LANES, LANES)
        bhi, blo = mat_hi[m, cut, :], mat_lo[m, cut, :]
        y = dot(rot_hi[slot], jnp.concatenate([bhi, blo], axis=0), ((1,), (1,)))
        return y[:, :LANES] + (y[:, LANES:] + dot(rot_lo[slot], bhi, ((1,), (1,))))

    def spread2(m, slot, i):
        cut = pl.ds(i * LANES, 2 * LANES)
        bhi, blo = mat_hi[m, cut, :], mat_lo[m, cut, :]
        hi = rot_hi[slot]
        y = dot(hi, bhi, ((1,), (1,))) + (dot(hi, blo, ((1,), (1,))) + dot(rot_lo[slot], bhi, ((1,), (1,))))
        return y[:, :LANES], y[:, LANES:]

    base = x * parents - half

    def tables():
        shape = (parents, nlist)
        row, slot = lax.broadcasted_iota(jnp.int32, shape, 0), lax.broadcasted_iota(jnp.int32, shape, 1)
        used = jnp.zeros(shape, jnp.int32)
        for b in range(parents):
            used = jnp.where(row == b, count[b], used)
        rows_o[...] = jnp.where(slot < used, rows_o[...], noff) * thetas
        p = jnp.maximum(rows_p[...] - base, 0)
        rows_p[...] = p * (pitch(1) // 8)
        idx_rows[...] = p * (pitch(len(inner)) // 8)

    idx_rows = slot_i[0]
    tabs = ((rows_p, slot_p), (idx_rows, slot_i[1]), (rows_o, slot_o))
    slot_i = slot_i[1]
    slots = [pltpu.make_async_copy(a, b, slot_sem.at[i]) for i, (a, b) in enumerate(tabs)]
    rim = [
        {
            "down": remote(rims.at[role], got.at[1], rim_send.at[0], rim_recv.at[0], "down"),
            "up": remote(rims.at[role], got.at[0], rim_send.at[1], rim_recv.at[1], "up"),
        }
        for role in (0, 1)
    ]

    def rim_out(role):
        rims[role] = spread(ends[role] * last, role * last, 2 * ends[role])
        when_do("down", rim[role]["down"], "start", ends[role] == 0)
        when_do("up", rim[role]["up"], "start", ends[role] == 1)

    def halo_in(role):
        when_do("down", to_up, "wait_recv", ends[role] == 0)
        when_do("up", to_down, "wait_recv", ends[role] == 1)
        gather(ends[role] * last, [tile(halo, ends[role])], 2 * ends[role], role, 0, False)
        boxes_out(role, 0)

    with jax.named_scope("k_tables"):
        tables()
    for copy in slots:
        copy.start()
    with jax.named_scope("k_inner"):
        for place, m in enumerate(inner):
            taps(m)
            gather(m, [tile(fine, k) for k in (m - 1, m, m + 1)], 0, len(roles), place, True)
            boxes_out(len(roles), place)
    with jax.named_scope("k_local"):
        for m in sorted({0, last}):
            taps(m)
        for role in roles:
            if thetas == 1:
                gather(0, [tile(fine, 0)], 1, 0, 0, True)
            else:
                k = ends[role] * (thetas - 2)
                gather(ends[role] * last, [tile(fine, k), tile(fine, k + 1)], 1 - ends[role], role, 0, True)
    if thetas == 1:
        when_do("down", to_up, "wait_recv")
        when_do("up", to_down, "wait_recv")
        gather(0, [tile(halo, 0)], 0, 0, 0, False)
        gather(0, [tile(halo, 1)], 2, 0, 0, False)
        boxes_out(0, 0)
    else:
        with jax.named_scope("k_halo0"):
            halo_in(0)
    for copy in slots:
        copy.wait()
    with jax.named_scope("k_trnwait"):
        load.wait()
    with jax.named_scope("k_boxin12"):
        for place, m in enumerate(inner):
            boxes_in(len(roles), place)
    with jax.named_scope("k_tr12"):
        prepare()
    if thetas > 1:
        with jax.named_scope("k_halo3"):
            halo_in(1)
    with jax.named_scope("k_boxin0"):
        boxes_in(0, 0)
    if thetas == 1:
        translate(0)
        rotate(0, 0)
        for role in (0, 1):
            rims[role] = spread(0, 0, 2 * role)
            when_do(("down", "up")[role], rim[role][("down", "up")[role]], "start")
        acc[0] = spread(0, 0, 1)
    else:
        with jax.named_scope("k_tr0"):
            translate(0)
        with jax.named_scope("k_rim0"):
            rotate(ends[0] * last, 0)
            rim_out(0)
        with jax.named_scope("k_spread12"):
            seen = set()

            def put(k, v):
                if k in seen:
                    acc[k] += v
                else:
                    acc[k] = v
                    seen.add(k)

            for m in inner:
                rotate(m, m)
                lo, mid = spread2(m, m, 0)
                put(m - 1, lo)
                put(m, mid)
                put(m + 1, spread(m, m, 2))
            for k in range(thetas):
                if k not in seen:
                    acc[k] = jnp.zeros(acc.shape[1:], jnp.float32)
        with jax.named_scope("k_boxin3"):
            boxes_in(1, 0)
        with jax.named_scope("k_tr3"):
            translate(1)
        with jax.named_scope("k_rim3"):
            rotate(ends[1] * last, last)
            rim_out(1)
        with jax.named_scope("k_rest"):
            for role in roles:
                k = ends[role] * (thetas - 2)
                lo, hi = spread2(ends[role] * last, role * last, 1 - ends[role])
                acc[k] += lo
                acc[k + 1] += hi

    @pl.when(d == 0)
    def _():
        got[0] = jnp.zeros(got.shape[1:], jnp.float32)

    @pl.when(d == nd - 1)
    def _():
        got[1] = jnp.zeros(got.shape[1:], jnp.float32)

    def result(k):
        for comp in range(2):
            for c in range(CHILDREN):
                rows = pl.ds((comp * CHILDREN + c) * parents, parents)
                v = acc[k, rows, :]
                if k == 0:
                    v = v + got[0, rows, :]
                if k == last:
                    v = v + got[1, rows, :]
                order[k, comp, pl.ds(c, parents, stride=CHILDREN), :] = v
        out[:, :, k * LANES : (k + 1) * LANES] = order[k]

    for k in inner:
        result(k)
    with jax.named_scope("k_rimA"):
        when_do("down", rim[0]["up"], "wait_recv", is_even)
        when_do("up", rim[0]["down"], "wait_recv", jnp.logical_not(is_even))
    with jax.named_scope("k_rimB"):
        when_do("down", rim[0]["up"], "wait_recv", jnp.logical_not(is_even))
        when_do("up", rim[0]["down"], "wait_recv", is_even)
    with jax.named_scope("k_end"):
        for k in sorted({0, last}):
            result(k)
    when_do("up", to_up, "wait_send")
    when_do("down", to_down, "wait_send")
    when_do("down", rim[0]["down"], "wait_send")
    when_do("up", rim[0]["up"], "wait_send")
    for group, g in enumerate(groups):
        for place in range(len(g)):
            for side in ("left", "right"):
                when_do(side, chunk(group, place, side), "wait_send")


VMEM = pl.BlockSpec(memory_space=pltpu.VMEM)
HBM = pl.BlockSpec(memory_space=pltpu.HBM)
MESH = pl.DeviceIdType.MESH


def shards(fine_out, interp_index, interp_weight, child_angle, translator, partners, offsets, list_count):
    _, children, cols = fine_out.shape
    parents = partners.shape[0]
    samples = child_angle.shape[1]
    noff = translator.shape[1]
    tiles = samples // LANES
    thetas = cols // LANES
    f32, bf16 = jnp.float32, jnp.bfloat16
    ordered = translator.reshape(2, noff, tiles, LANES).transpose(1, 2, 0, 3).reshape(noff * thetas, 8, LANES)
    dma = pltpu.SemaphoreType.DMA
    groups = [1] * min(thetas, 2) + ([thetas - 2] if thetas > 2 else [])
    operands = (partners, offsets, list_count, fine_out, interp_index.T, interp_weight.T, child_angle, ordered)
    return pl.pallas_call(
        kernel,
        out_shape=jax.ShapeDtypeStruct((2, children, cols), f32),
        in_specs=[HBM] * 8,
        out_specs=VMEM,
        scratch_shapes=[
            pltpu.SMEM(list_count.shape, jnp.int32),
            pltpu.VMEM(partners.shape, jnp.int32),
            pltpu.VMEM(offsets.shape, jnp.int32),
            pltpu.SMEM(partners.shape, jnp.int32),
            (pltpu.VMEM(partners.shape, jnp.int32), pltpu.SMEM(partners.shape, jnp.int32)),
            pltpu.SMEM(offsets.shape, jnp.int32),
            pltpu.VMEM((thetas, 2, children, LANES), f32),
            pltpu.VMEM((TAPS, samples), jnp.int32),
            pltpu.VMEM((TAPS, samples), f32),
            pltpu.VMEM(child_angle.shape, f32),
            pltpu.VMEM((thetas, CHILDREN, 4 * LANES), f32),
            pltpu.VMEM((thetas, CHILDREN, 4 * LANES), f32),
            dma((thetas,)),
            dma((6,)),
            dma((3,)),
            pltpu.VMEM((2, 2, children, LANES), f32),
            pltpu.VMEM((thetas, 3 * LANES, 4 * LANES), bf16),
            pltpu.VMEM((thetas, 3 * LANES, 4 * LANES), bf16),
            [pltpu.VMEM((2 * parents * pitch(n) // 8, 8, LANES), f32) for n in groups],
            pltpu.VMEM(((noff + 1) * thetas, 8, LANES), f32),
            pltpu.VMEM((min(thetas, 2), parents * partners.shape[1], 8, LANES), f32),
            pltpu.VMEM((thetas, parents, pitch(1), LANES), f32),
            pltpu.VMEM((thetas, 2 * children, 4 * LANES), bf16),
            pltpu.VMEM((thetas, 2 * children, 4 * LANES), bf16),
            pltpu.VMEM((thetas, 2 * children, LANES), f32),
            pltpu.VMEM((2, 2 * children, LANES), f32),
            pltpu.VMEM((2, 2 * children, LANES), f32),
            pltpu.VMEM((thetas, 2, children, LANES), f32),
            dma((2,)), dma((2,)), dma((2, thetas)), dma((2, thetas)), dma((2,)), dma((2,)), dma,
        ],
        compiler_params=pltpu.CompilerParams(
            vmem_limit_bytes=40 * 1024 * 1024, collective_id=0, has_side_effects=True
        ),
    )(*(pltpu.with_memory_space_constraint(v, pltpu.HBM) for v in operands))


def solution(mesh):
    placed = (
        P(None, "box", "dir"),
        P("dir", None),
        P("dir", None),
        P(None, "dir"),
        P(None, None, "dir"),
        P("box", None),
        P("box", None),
        P("box"),
    )
    return jax.shard_map(
        shards, mesh=mesh, in_specs=placed, out_specs=P(None, "box", "dir"), check_vma=False
    )
```

```python
import functools

import jax
import jax.numpy as jnp
from jax import lax
from jax.experimental import pallas as pl
from jax.experimental.pallas import tpu as pltpu
from jax.sharding import PartitionSpec as P

LANES = 128
TAPS = 4
CHILDREN = 4


def pitch(rows):
    return 16 * rows + 8


def split(x):
    hi = x.astype(jnp.bfloat16)
    return hi, (x - hi.astype(jnp.float32)).astype(jnp.bfloat16)


def dot(a, b, dims):
    return lax.dot_general(a, b, dimension_numbers=(dims, ((), ())), preferred_element_type=jnp.float32)


def kernel(
    partners_in, offsets_in, count_in, fine_in, idx_in, w_in, angle_in, translator, out,
    count, rows_p, rows_o, slot_p, slot_i, slot_o, fine, idx, w, angle, cos, sin, fine_sem, in_sem, slot_sem, halo,
    mat_hi, mat_lo, srcs, trn, pre, par, rot_hi, rot_lo, acc, rims, got, order,
    halo_send, halo_recv, box_send, box_recv, rim_send, rim_recv, trn_sem,
):
    thetas, _, children, _ = fine.shape
    parents = children // CHILDREN
    half = parents // 2
    some = CHILDREN * half
    tiles = angle.shape[1] // LANES
    noff = translator.shape[0] // thetas
    nlist = rows_p.shape[1]
    width = 4 * LANES
    last = thetas - 1
    inner = tuple(range(1, last))
    roles = (0, 1) if thetas > 1 else (0,)
    d, nd = lax.axis_index("dir"), lax.axis_size("dir")
    x, nx = lax.axis_index("box"), lax.axis_size("box")
    has = {"down": d > 0, "up": d < nd - 1, "left": x > 0, "right": x < nx - 1}
    ids = {"down": {"dir": d - 1}, "up": {"dir": d + 1}, "left": {"box": x - 1}, "right": {"box": x + 1}}
    is_even = d % 2 == 0
    top = jnp.where(is_even, 0, 1)
    ends = (top, 1 - top)

    fine_loads = {
        k: pltpu.make_async_copy(fine_in.at[:, :, pl.ds(k * LANES, LANES)], fine.at[k], fine_sem.at[k])
        for k in (*sorted({0, last}), *inner)
    }
    pairs = ((idx_in, idx), (w_in, w), (angle_in, angle), (partners_in, rows_p), (offsets_in, rows_o), (count_in, count))
    loads = [pltpu.make_async_copy(a, b, in_sem.at[i]) for i, (a, b) in enumerate(pairs)]
    for copy in (*fine_loads.values(), *loads):
        copy.start()
    load = pltpu.make_async_copy(translator, trn.at[pl.ds(0, noff * thetas)], trn_sem)
    load.start()

    barrier = pltpu.get_barrier_semaphore()
    for side in ids:
        @pl.when(has[side])
        def _(side=side):
            pl.semaphore_signal(barrier, inc=1, device_id=ids[side], device_id_type=MESH)
    pl.semaphore_wait(barrier, sum(jnp.where(here, 1, 0) for here in has.values()))

    def remote(source, target, send, recv, side):
        return pltpu.make_async_remote_copy(
            src_ref=source, dst_ref=target, send_sem=send, recv_sem=recv,
            device_id=ids[side], device_id_type=MESH,
        )

    def when_do(side, copy, act, also=None):
        @pl.when(has[side] if also is None else jnp.logical_and(has[side], also))
        def _():
            getattr(copy, act)()

    def by_side(body):
        for n in (0, 1):
            @pl.when(x % 2 == n)
            def _(n=n):
                body(n)

    def halo_copy(side, h):
        n, k = (0, last) if side == "up" else (1, 0)
        rows = pl.ds(h * some, some)
        return remote(fine.at[k, :, rows], halo.at[n, :, rows], halo_send.at[n, h], halo_recv.at[n, h], side)

    for k in sorted({0, last}):
        fine_loads[k].wait()
    @by_side
    def _(far):
        for h in (far, 1 - far):
            for side in ("up", "down"):
                when_do(side, halo_copy(side, h), "start")

    @pl.when(d == 0)
    def _():
        halo[0] = jnp.zeros(halo.shape[1:], jnp.float32)

    @pl.when(d == nd - 1)
    def _():
        halo[1] = jnp.zeros(halo.shape[1:], jnp.float32)

    mid = srcs[2 * len(roles)] if inner else None
    ranges = half + parents

    def boxed(ref, rows=1):
        return ref.reshape(ref.shape[0] * 8 // pitch(rows), pitch(rows), LANES)

    def flat(ref):
        return ref.reshape(ref.shape[0] * 8, LANES)

    def ends_src(role, h):
        return srcs[2 * role + h]

    @pl.when(x == 0)
    def _():
        for role in roles:
            boxed(ends_src(role, 0))[:half] = jnp.zeros((half, pitch(1), LANES), jnp.float32)
        if inner:
            boxed(mid, len(inner))[:half] = jnp.zeros((half, pitch(len(inner)), LANES), jnp.float32)

    @pl.when(x == nx - 1)
    def _():
        for role in roles:
            boxed(ends_src(role, 1))[parents:] = jnp.zeros((half, pitch(1), LANES), jnp.float32)
        if inner:
            boxed(mid, len(inner))[half + parents :] = jnp.zeros((half, pitch(len(inner)), LANES), jnp.float32)

    trn[noff * thetas :] = jnp.zeros((thetas, 8, LANES), jnp.float32)
    for copy in loads:
        copy.wait()
    for k in inner:
        fine_loads[k].wait()
    first = d * thetas * LANES
    for m in range(thetas):
        cos[m] = jnp.cos(angle[:, m * width : (m + 1) * width])
        sin[m] = jnp.sin(angle[:, m * width : (m + 1) * width])

    def taps(m):
        position = lax.broadcasted_iota(jnp.int32, (3 * LANES, width), 0) + (first + (m - 1) * LANES)
        total = jnp.zeros((3 * LANES, width), jnp.float32)
        for t in range(TAPS):
            at = idx[t : t + 1, m * width : (m + 1) * width]
            total = total + jnp.where(at == position, w[t : t + 1, m * width : (m + 1) * width], 0.0)
        mat_hi[m], mat_lo[m] = split(total)

    def tile(ref, k, halves=(0, 1)):
        return split(jnp.concatenate(
            [
                ref[k, comp, pl.ds(h * some + c, half, stride=CHILDREN), :]
                for h in halves for comp in range(2) for c in range(CHILDREN)
            ],
            axis=0,
        ))

    def gather(m, tiles, start, places, fresh, halves=(0, 1)):
        hi, lo = [v[0] for v in tiles], [v[1] for v in tiles]
        cut = pl.ds(start * LANES, len(tiles) * LANES)
        bhi, blo = mat_hi[m, cut, :], mat_lo[m, cut, :]
        y = dot(jnp.concatenate(hi + lo + hi, axis=1), jnp.concatenate([bhi, bhi, blo], axis=0), ((1,), (0,)))
        for i in range(4):
            cut = pl.ds(i * LANES, LANES)
            phases = [(cos[m, pl.ds(c, 1), cut], sin[m, pl.ds(c, 1), cut]) for c in range(CHILDREN)]
            for n, h in enumerate(halves):
                re = im = None
                for c, (cc, sc) in enumerate(phases):
                    at = 2 * n * some + c * half
                    xr = y[at : at + half, i * LANES : (i + 1) * LANES]
                    xi = y[at + some : at + some + half, i * LANES : (i + 1) * LANES]
                    r, j = xr * cc - xi * sc, xr * sc + xi * cc
                    re, im = (r, j) if c == 0 else (re + r, im + j)

                def own(place, row):
                    return pl.ds(place[2] + h * half * place[1] + 2 * i + row, half, stride=place[1])

                if not fresh:
                    place = places[0]
                    re, im = re + place[0][own(place, 0), :], im + place[0][own(place, 1), :]
                for place in places:
                    for row, v in ((0, re), (1, im), (8, im), (9, re)):
                        place[0][own(place, row), :] = v

    def end_places(role):
        return [(flat(ends_src(role, 0)), pitch(1), half * pitch(1)), (flat(ends_src(role, 1)), pitch(1), 0)]

    def exchange(source, target, first, rows, sem, side):
        return remote(
            source.at[pl.ds(first, half), rows, :], target[0].at[pl.ds(target[1], half), rows, :],
            box_send.at[sem], box_recv.at[sem], side,
        )

    def end_chunk(role, side):
        rows = pl.ds(0, 8)
        if side == "left":
            return exchange(boxed(ends_src(role, 1)), (boxed(ends_src(role, 1)), parents), 0, rows, (0, role * last), side)
        return exchange(boxed(ends_src(role, 0)), (boxed(ends_src(role, 0)), 0), parents, rows, (1, role * last), side)

    def mid_chunk(place, side):
        rows, ref = pl.ds(16 * place, 8), boxed(mid, len(inner))
        if side == "left":
            return exchange(ref, (ref, half + parents), half, rows, (0, inner[place]), side)
        return exchange(ref, (ref, 0), parents, rows, (1, inner[place]), side)

    even = lax.broadcasted_iota(jnp.int32, (8, LANES), 0) % 2 == 0

    def swap(ref, boxes, place):
        for p in boxes:
            v = ref[p, 16 * place : 16 * place + 8, :]
            ref[p, 16 * place + 8 : 16 * place + 16, :] = jnp.where(even, pltpu.roll(v, 7, 0), pltpu.roll(v, 1, 0))

    def sums(slots, n):
        one, two = {}, {}
        for s, (t, u, v) in enumerate(slots):
            u, v = t * u, t * v
            one[s % n], two[s % n] = (u, v) if s < n else (one[s % n] + u, two[s % n] + v)
        n = min(n, len(one))
        return sum(one[k] for k in range(n)), sum(two[k] for k in range(n))

    def prepare():
        for b in range(parents):
            for s in range(nlist):
                o = slot_o[b, s]
                for role in roles:
                    pre[role, b * nlist + s] = trn[o + role * last]

    def translate_inner(boxes):
        for b in boxes if inner else ():
            made = {m: [] for m in inner}
            for s in range(nlist):
                o, p = slot_o[b, s], slot_i[b, s]
                for place, m in enumerate(inner):
                    made[m].append((trn[o + m], mid[p + 2 * place], mid[p + 2 * place + 1]))
            for m in inner:
                par[m, b, 0:8, :], par[m, b, 8:16, :] = sums(made[m], 1)

    def translate(role, h):
        src = ends_src(role, h)
        m = ends[role] if thetas > 1 else 0
        if h == 0:
            when_do("left", end_chunk(role, "right"), "wait_recv")
            swap(boxed(src), range(half), 0)
        else:
            when_do("right", end_chunk(role, "left"), "wait_recv")
            swap(boxed(src), range(parents, parents + half), 0)
        for b in range(h * half, (h + 1) * half):
            made = []
            for s in range(nlist):
                p = slot_p[b, s]
                made.append((pre[m, b * nlist + s], src[p], src[p + 1]))
            par[role * last, b, 0:8, :], par[role * last, b, 8:16, :] = sums(made, 2)

    par2 = par.reshape(thetas * parents * pitch(1), LANES)

    def rotate(m, slot, h):
        def part(row):
            return par2[pl.ds((slot * parents + h * half) * pitch(1) + row, half, stride=pitch(1)), :]

        pr = jnp.concatenate([part(2 * i) - part(2 * i + 1) for i in range(4)], axis=1)
        pi = jnp.concatenate([part(8 + 2 * i) + part(9 + 2 * i) for i in range(4)], axis=1)
        for c in range(CHILDREN):
            cc, sc = cos[m, pl.ds(c, 1), :], sin[m, pl.ds(c, 1), :]
            for comp, v in enumerate((pr * cc + pi * sc, pi * cc - pr * sc)):
                rows = pl.ds((2 * h + comp) * some + c * half, half)
                rot_hi[slot, rows, :], rot_lo[slot, rows, :] = split(v)

    def spread(m, slot, i, rows):
        cut = pl.ds(i * LANES, LANES)
        bhi, blo = mat_hi[m, cut, :], mat_lo[m, cut, :]
        y = dot(rot_hi[slot, rows, :], jnp.concatenate([bhi, blo], axis=0), ((1,), (1,)))
        return y[:, :LANES] + (y[:, LANES:] + dot(rot_lo[slot, rows, :], bhi, ((1,), (1,))))

    def spread2(m, slot, i):
        cut = pl.ds(i * LANES, 2 * LANES)
        bhi, blo = mat_hi[m, cut, :], mat_lo[m, cut, :]
        hi = rot_hi[slot]
        y = dot(hi, bhi, ((1,), (1,))) + (dot(hi, blo, ((1,), (1,))) + dot(rot_lo[slot], bhi, ((1,), (1,))))
        return y[:, :LANES], y[:, LANES:]

    def tables():
        shape = (parents, nlist)
        row, slot = lax.broadcasted_iota(jnp.int32, shape, 0), lax.broadcasted_iota(jnp.int32, shape, 1)
        used = jnp.zeros(shape, jnp.int32)
        for b in range(parents):
            used = jnp.where(row == b, count[b], used)
        rows_o[...] = jnp.where(slot < used, rows_o[...], noff) * thetas
        p = rows_p[...] - (x * parents - half)
        near = p - jnp.where(row < half, 0, half)
        idx_rows[...] = jnp.clip(p, 0, 2 * parents - 1) * (pitch(len(inner)) // 8)
        rows_p[...] = jnp.clip(near, 0, ranges - 1) * (pitch(1) // 8)

    idx_rows = slot_i[0]
    tabs = ((rows_p, slot_p), (idx_rows, slot_i[1]), (rows_o, slot_o))
    slot_i = slot_i[1]
    slots = [pltpu.make_async_copy(a, b, slot_sem.at[i]) for i, (a, b) in enumerate(tabs)]

    def rim_copy(role, side, h):
        n = 1 if side == "down" else 0
        return remote(rims.at[role, h], got.at[n, h], rim_send.at[n, h], rim_recv.at[n, h], side)

    def rim_out(role, h):
        m = ends[role] * last
        rotate(m, role * last, h)
        rims[role, h] = spread(m, role * last, 2 * ends[role], pl.ds(2 * h * some, 2 * some))
        when_do("down", rim_copy(role, "down", h), "start", ends[role] == 0)
        when_do("up", rim_copy(role, "up", h), "start", ends[role] == 1)

    def halo_in(role, h):
        when_do("down", halo_copy("up", h), "wait_recv", ends[role] == 0)
        when_do("up", halo_copy("down", h), "wait_recv", ends[role] == 1)
        gather(ends[role] * last, [tile(halo, ends[role], (h,))], 2 * ends[role], end_places(role), False, (h,))
        side = ("left", "right")[h]
        when_do(side, end_chunk(role, side), "start")

    with jax.named_scope("k_tables"):
        tables()
    for copy in slots:
        copy.start()
    everything = pl.ds(0, 4 * some)
    with jax.named_scope("k_inner"):
        for place, m in enumerate(inner):
            taps(m)
            where = (flat(mid), pitch(len(inner)), half * pitch(len(inner)) + 16 * place)
            gather(m, [tile(fine, k) for k in (m - 1, m, m + 1)], 0, [where], True)
            for side in ("left", "right"):
                when_do(side, mid_chunk(place, side), "start")
    with jax.named_scope("k_local"):
        for m in sorted({0, last}):
            taps(m)
        for role in roles:
            if thetas == 1:
                gather(0, [tile(fine, 0)], 1, end_places(0)[:1], True)
            else:
                k = ends[role] * (thetas - 2)
                gather(ends[role] * last, [tile(fine, k), tile(fine, k + 1)], 1 - ends[role], end_places(role)[:1], True)
    for copy in slots:
        copy.wait()
    with jax.named_scope("k_trnwait"):
        load.wait()
    with jax.named_scope("k_pre"):
        prepare()
    def first_halos(far):
        for h in (far, 1 - far):
            if thetas == 1:
                when_do("down", halo_copy("up", h), "wait_recv")
                when_do("up", halo_copy("down", h), "wait_recv")
                gather(0, [tile(halo, 0, (h,))], 0, end_places(0)[:1], False, (h,))
                gather(0, [tile(halo, 1, (h,))], 2, end_places(0), False, (h,))
                side = ("left", "right")[h]
                when_do(side, end_chunk(0, side), "start")
            else:
                halo_in(0, h)

    def first_end(far):
        for h in (1 - far, far):
            with jax.named_scope("k_tr0_%d" % (h == far)):
                translate(0, h)
            with jax.named_scope("k_rim0_%d" % (h == far)):
                if thetas > 1:
                    rim_out(0, h)
                else:
                    rotate(0, 0, h)
                    for n, side in enumerate(("down", "up")):
                        rims[n, h] = spread(0, 0, 2 * n, pl.ds(2 * h * some, 2 * some))
                        when_do(side, rim_copy(n, side, h), "start")
            if thetas > 1 and h != far:
                with jax.named_scope("k_halo3_0"):
                    halo_in(1, far)
                with jax.named_scope("k_halo3_1"):
                    halo_in(1, 1 - far)

    def second_end(far):
        for h in (1 - far, far):
            with jax.named_scope("k_tr3_%d" % (h == far)):
                translate(1, h)
            with jax.named_scope("k_rim3_%d" % (h == far)):
                rim_out(1, h)

    with jax.named_scope("k_halo0"):
        by_side(first_halos)
    with jax.named_scope("k_boxin12"):
        for place, m in enumerate(inner):
            when_do("right", mid_chunk(place, "left"), "wait_recv")
            when_do("left", mid_chunk(place, "right"), "wait_recv")
            swap(boxed(mid, len(inner)), (*range(half), *range(half + parents, 2 * parents)), place)
    with jax.named_scope("k_tr12a"):
        translate_inner(range(half))
    by_side(first_end)
    if thetas == 1:
        acc[0] = spread(0, 0, 1, everything)
    else:
        by_side(second_end)
        with jax.named_scope("k_tr12b"):
            translate_inner(range(half, parents))
        with jax.named_scope("k_spread12"):
            seen = set()

            def put(k, v):
                if k in seen:
                    acc[k] += v
                else:
                    acc[k] = v
                    seen.add(k)

            for m in inner:
                for h in (0, 1):
                    rotate(m, m, h)
                lo, middle = spread2(m, m, 0)
                put(m - 1, lo)
                put(m, middle)
                put(m + 1, spread(m, m, 2, everything))
            for k in range(thetas):
                if k not in seen:
                    acc[k] = jnp.zeros(acc.shape[1:], jnp.float32)
        with jax.named_scope("k_rest"):
            for role in roles:
                k = ends[role] * (thetas - 2)
                lo, hi = spread2(ends[role] * last, role * last, 1 - ends[role])
                acc[k] += lo
                acc[k + 1] += hi

    @pl.when(d == 0)
    def _():
        got[0] = jnp.zeros(got.shape[1:], jnp.float32)

    @pl.when(d == nd - 1)
    def _():
        got[1] = jnp.zeros(got.shape[1:], jnp.float32)

    def result(k):
        for h in (0, 1):
            for comp in range(2):
                for c in range(CHILDREN):
                    at = comp * some + c * half
                    v = acc[k, pl.ds(2 * h * some + at, half), :]
                    if k == 0:
                        v = v + got[0, h, pl.ds(at, half), :]
                    if k == last:
                        v = v + got[1, h, pl.ds(at, half), :]
                    order[k, comp, pl.ds(h * some + c, half, stride=CHILDREN), :] = v
        out[:, :, k * LANES : (k + 1) * LANES] = order[k]

    for k in inner:
        result(k)
    with jax.named_scope("k_rimA"):
        for h in (1, 0):
            when_do("down", rim_copy(0, "up", h), "wait_recv", is_even)
            when_do("up", rim_copy(0, "down", h), "wait_recv", jnp.logical_not(is_even))
    with jax.named_scope("k_rimB"):
        for h in (1, 0):
            when_do("down", rim_copy(0, "up", h), "wait_recv", jnp.logical_not(is_even))
            when_do("up", rim_copy(0, "down", h), "wait_recv", is_even)
    with jax.named_scope("k_end"):
        for k in sorted({0, last}):
            result(k)
    for h in (0, 1):
        for side in ("up", "down"):
            when_do(side, halo_copy(side, h), "wait_send")
            when_do(side, rim_copy(0, side, h), "wait_send")
    for side in ("left", "right"):
        for role in roles:
            when_do(side, end_chunk(role, side), "wait_send")
        for place in range(len(inner)):
            when_do(side, mid_chunk(place, side), "wait_send")


VMEM = pl.BlockSpec(memory_space=pltpu.VMEM)
HBM = pl.BlockSpec(memory_space=pltpu.HBM)
MESH = pl.DeviceIdType.MESH


def shards(fine_out, interp_index, interp_weight, child_angle, translator, partners, offsets, list_count):
    _, children, cols = fine_out.shape
    parents = partners.shape[0]
    samples = child_angle.shape[1]
    noff = translator.shape[1]
    tiles = samples // LANES
    thetas = cols // LANES
    f32, bf16 = jnp.float32, jnp.bfloat16
    ordered = translator.reshape(2, noff, tiles, LANES).transpose(1, 2, 0, 3).reshape(noff * thetas, 8, LANES)
    dma = pltpu.SemaphoreType.DMA
    operands = (partners, offsets, list_count, fine_out, interp_index.T, interp_weight.T, child_angle, ordered)
    return pl.pallas_call(
        kernel,
        out_shape=jax.ShapeDtypeStruct((2, children, cols), f32),
        in_specs=[HBM] * 8,
        out_specs=VMEM,
        scratch_shapes=[
            pltpu.SMEM(list_count.shape, jnp.int32),
            pltpu.VMEM(partners.shape, jnp.int32),
            pltpu.VMEM(offsets.shape, jnp.int32),
            pltpu.SMEM(partners.shape, jnp.int32),
            (pltpu.VMEM(partners.shape, jnp.int32), pltpu.SMEM(partners.shape, jnp.int32)),
            pltpu.SMEM(offsets.shape, jnp.int32),
            pltpu.VMEM((thetas, 2, children, LANES), f32),
            pltpu.VMEM((TAPS, samples), jnp.int32),
            pltpu.VMEM((TAPS, samples), f32),
            pltpu.VMEM(child_angle.shape, f32),
            pltpu.VMEM((thetas, CHILDREN, 4 * LANES), f32),
            pltpu.VMEM((thetas, CHILDREN, 4 * LANES), f32),
            dma((thetas,)),
            dma((6,)),
            dma((3,)),
            pltpu.VMEM((2, 2, children, LANES), f32),
            pltpu.VMEM((thetas, 3 * LANES, 4 * LANES), bf16),
            pltpu.VMEM((thetas, 3 * LANES, 4 * LANES), bf16),
            [pltpu.VMEM((parents * 3 // 2 * pitch(1) // 8, 8, LANES), f32)] * (2 * min(thetas, 2))
            + [pltpu.VMEM((2 * parents * pitch(thetas - 2) // 8, 8, LANES), f32)] * (thetas > 2),
            pltpu.VMEM(((noff + 1) * thetas, 8, LANES), f32),
            pltpu.VMEM((min(thetas, 2), parents * partners.shape[1], 8, LANES), f32),
            pltpu.VMEM((thetas, parents, pitch(1), LANES), f32),
            pltpu.VMEM((thetas, 2 * children, 4 * LANES), bf16),
            pltpu.VMEM((thetas, 2 * children, 4 * LANES), bf16),
            pltpu.VMEM((thetas, 2 * children, LANES), f32),
            pltpu.VMEM((2, 2, children, LANES), f32),
            pltpu.VMEM((2, 2, children, LANES), f32),
            pltpu.VMEM((thetas, 2, children, LANES), f32),
            dma((2, 2)), dma((2, 2)), dma((2, thetas)), dma((2, thetas)), dma((2, 2)), dma((2, 2)), dma,
        ],
        compiler_params=pltpu.CompilerParams(
            vmem_limit_bytes=40 * 1024 * 1024, collective_id=0, has_side_effects=True
        ),
    )(*(pltpu.with_memory_space_constraint(v, pltpu.HBM) for v in operands))


def solution(mesh):
    placed = (
        P(None, "box", "dir"),
        P("dir", None),
        P("dir", None),
        P(None, "dir"),
        P(None, None, "dir"),
        P("box", None),
        P("box", None),
        P("box"),
    )
    return jax.shard_map(
        shards, mesh=mesh, in_specs=placed, out_specs=P(None, "box", "dir"), check_vma=False
    )
```

```python
import functools

import jax
import jax.numpy as jnp
from jax import lax
from jax.experimental import pallas as pl
from jax.experimental.pallas import tpu as pltpu
from jax.sharding import PartitionSpec as P

LANES = 128
TAPS = 4
CHILDREN = 4


def pitch(rows):
    return 16 * rows + 8


def split(x):
    hi = x.astype(jnp.bfloat16)
    return hi, (x - hi.astype(jnp.float32)).astype(jnp.bfloat16)


def dot(a, b, dims):
    return lax.dot_general(a, b, dimension_numbers=(dims, ((), ())), preferred_element_type=jnp.float32)


def kernel(
    partners_in, offsets_in, count_in, fine_in, idx_in, w_in, angle_in, translator, out,
    count, rows_p, rows_o, slot_p, slot_i, slot_o, fine, idx, w, angle, cos, sin, fine_sem, halo,
    mat_hi, mat_lo, srcs, trn, pre, par, rot_hi, rot_lo, acc, rims, got, order,
    sent, halo_recv, box_recv, rim_recv, trn_sem,
):
    thetas, _, children, _ = fine.shape
    parents = children // CHILDREN
    half = parents // 2
    some = CHILDREN * half
    tiles = angle.shape[1] // LANES
    noff = translator.shape[0] // thetas
    nlist = rows_p.shape[1]
    width = 4 * LANES
    last = thetas - 1
    inner = tuple(range(1, last))
    roles = (0, 1) if thetas > 1 else (0,)
    d, nd = lax.axis_index("dir"), lax.axis_size("dir")
    x, nx = lax.axis_index("box"), lax.axis_size("box")
    has = {"down": d > 0, "up": d < nd - 1, "left": x > 0, "right": x < nx - 1}
    ids = {"down": {"dir": d - 1}, "up": {"dir": d + 1}, "left": {"box": x - 1}, "right": {"box": x + 1}}
    is_even = d % 2 == 0
    top = jnp.where(is_even, 0, 1)
    ends = (top, 1 - top)

    fine_loads = {
        k: pltpu.make_async_copy(fine_in.at[:, :, pl.ds(k * LANES, LANES)], fine.at[k], fine_sem.at[0 if k in (0, last) else 1])
        for k in (*sorted({0, last}), *inner)
    }
    pairs = ((idx_in, idx), (w_in, w), (angle_in, angle), (partners_in, rows_p), (offsets_in, rows_o), (count_in, count))
    loads = [pltpu.make_async_copy(a, b, fine_sem.at[1]) for a, b in pairs]
    for copy in (*fine_loads.values(), *loads):
        copy.start()
    load = pltpu.make_async_copy(translator, trn.at[pl.ds(0, noff * thetas)], trn_sem)
    load.start()

    barrier = pltpu.get_barrier_semaphore()
    for side in ids:
        @pl.when(has[side])
        def _(side=side):
            pl.semaphore_signal(barrier, inc=1, device_id=ids[side], device_id_type=MESH)
    pl.semaphore_wait(barrier, sum(jnp.where(here, 1, 0) for here in has.values()))

    def remote(source, target, send, recv, side):
        return pltpu.make_async_remote_copy(
            src_ref=source, dst_ref=target, send_sem=send, recv_sem=recv,
            device_id=ids[side], device_id_type=MESH,
        )

    def when_do(side, copy, act, also=None):
        @pl.when(has[side] if also is None else jnp.logical_and(has[side], also))
        def _():
            getattr(copy, act)()

    def by_side(body):
        for n in (0, 1):
            @pl.when(x % 2 == n)
            def _(n=n):
                body(n)

    def halo_copy(side, h):
        n, k = (0, last) if side == "up" else (1, 0)
        rows = pl.ds(h * some, some)
        return remote(fine.at[k, :, rows], halo.at[n, :, rows], sent.at[n], halo_recv.at[n, h], side)

    for k in sorted({0, last}):
        fine_loads[k].wait()
    @by_side
    def _(far):
        for h in (1 - far, far):
            for side in ("up", "down"):
                when_do(side, halo_copy(side, h), "start")

    @pl.when(d == 0)
    def _():
        halo[0] = jnp.zeros(halo.shape[1:], jnp.float32)

    @pl.when(d == nd - 1)
    def _():
        halo[1] = jnp.zeros(halo.shape[1:], jnp.float32)

    mid = srcs[2 * len(roles)] if inner else None
    ranges = half + parents

    def boxed(ref, rows=1):
        return ref.reshape(ref.shape[0] * 8 // pitch(rows), pitch(rows), LANES)

    def flat(ref):
        return ref.reshape(ref.shape[0] * 8, LANES)

    def ends_src(role, h):
        return srcs[2 * role + h]

    @pl.when(x == 0)
    def _():
        for role in roles:
            boxed(ends_src(role, 0))[:half] = jnp.zeros((half, pitch(1), LANES), jnp.float32)
        if inner:
            boxed(mid, len(inner))[:half] = jnp.zeros((half, pitch(len(inner)), LANES), jnp.float32)

    @pl.when(x == nx - 1)
    def _():
        for role in roles:
            boxed(ends_src(role, 1))[parents:] = jnp.zeros((half, pitch(1), LANES), jnp.float32)
        if inner:
            boxed(mid, len(inner))[half + parents :] = jnp.zeros((half, pitch(len(inner)), LANES), jnp.float32)

    trn[noff * thetas :] = jnp.zeros((thetas, 8, LANES), jnp.float32)
    for copy in (*loads, *(fine_loads[k] for k in inner)):
        copy.wait()
    first = d * thetas * LANES
    for m in range(thetas):
        cos[m] = jnp.cos(angle[:, m * width : (m + 1) * width])
        sin[m] = jnp.sin(angle[:, m * width : (m + 1) * width])

    def taps(m):
        position = lax.broadcasted_iota(jnp.int32, (3 * LANES, width), 0) + (first + (m - 1) * LANES)
        total = jnp.zeros((3 * LANES, width), jnp.float32)
        for t in range(TAPS):
            at = idx[t : t + 1, m * width : (m + 1) * width]
            total = total + jnp.where(at == position, w[t : t + 1, m * width : (m + 1) * width], 0.0)
        mat_hi[m], mat_lo[m] = split(total)

    def tile(ref, k, halves=(0, 1)):
        return split(jnp.concatenate(
            [
                ref[k, comp, pl.ds(h * some + c, half, stride=CHILDREN), :]
                for h in halves for comp in range(2) for c in range(CHILDREN)
            ],
            axis=0,
        ))

    def gather(m, tiles, start, places, fresh, halves=(0, 1)):
        hi, lo = [v[0] for v in tiles], [v[1] for v in tiles]
        cut = pl.ds(start * LANES, len(tiles) * LANES)
        bhi, blo = mat_hi[m, cut, :], mat_lo[m, cut, :]
        y = dot(jnp.concatenate(hi + lo + hi, axis=1), jnp.concatenate([bhi, bhi, blo], axis=0), ((1,), (0,)))
        for i in range(4):
            cut = pl.ds(i * LANES, LANES)
            phases = [(cos[m, pl.ds(c, 1), cut], sin[m, pl.ds(c, 1), cut]) for c in range(CHILDREN)]
            for n, h in enumerate(halves):
                re = im = None
                for c, (cc, sc) in enumerate(phases):
                    at = 2 * n * some + c * half
                    xr = y[at : at + half, i * LANES : (i + 1) * LANES]
                    xi = y[at + some : at + some + half, i * LANES : (i + 1) * LANES]
                    r, j = xr * cc - xi * sc, xr * sc + xi * cc
                    re, im = (r, j) if c == 0 else (re + r, im + j)

                def own(place, row):
                    return pl.ds(place[2] + h * half * place[1] + 2 * i + row, half, stride=place[1])

                if not fresh:
                    place = places[0]
                    re, im = re + place[0][own(place, 0), :], im + place[0][own(place, 1), :]
                for place in places:
                    for row, v in ((0, re), (1, im), (8, im), (9, re)):
                        place[0][own(place, row), :] = v

    def end_places(role):
        return [(flat(ends_src(role, 0)), pitch(1), half * pitch(1)), (flat(ends_src(role, 1)), pitch(1), 0)]

    def exchange(source, target, first, rows, sem, side):
        return remote(
            source.at[pl.ds(first, half), rows, :], target[0].at[pl.ds(target[1], half), rows, :],
            sent.at[2 if side == "left" else 3], box_recv.at[sem], side,
        )

    def end_chunk(role, side):
        rows = pl.ds(0, 8)
        if side == "left":
            return exchange(boxed(ends_src(role, 1)), (boxed(ends_src(role, 1)), parents), 0, rows, 2 + 2 * role, side)
        return exchange(boxed(ends_src(role, 0)), (boxed(ends_src(role, 0)), 0), parents, rows, 3 + 2 * role, side)

    def mid_chunk(rows, side):
        ref = boxed(mid, len(inner))
        if side == "left":
            return exchange(ref, (ref, half + parents), half, rows, 0, side)
        return exchange(ref, (ref, 0), parents, rows, 1, side)

    def all_sent():
        when_do("up", remote(rims, got, sent.at[0], rim_recv.at[0], "up"), "wait_send")
        when_do("down", remote(rims, got, sent.at[1], rim_recv.at[1], "down"), "wait_send")
        ref, rows = boxed(mid, len(inner)) if inner else boxed(ends_src(0, 0)), pl.ds(0, 8 * thetas)
        for side in ("left", "right"):
            when_do(side, exchange(ref, (ref, half), 0, rows, 0, side), "wait_send")

    even = lax.broadcasted_iota(jnp.int32, (8, LANES), 0) % 2 == 0

    def swap(ref, boxes, place):
        for p in boxes:
            v = ref[p, 16 * place : 16 * place + 8, :]
            ref[p, 16 * place + 8 : 16 * place + 16, :] = jnp.where(even, pltpu.roll(v, 7, 0), pltpu.roll(v, 1, 0))

    def sums(slots, n):
        one, two = {}, {}
        for s, (t, u, v) in enumerate(slots):
            u, v = t * u, t * v
            one[s % n], two[s % n] = (u, v) if s < n else (one[s % n] + u, two[s % n] + v)
        n = min(n, len(one))
        return sum(one[k] for k in range(n)), sum(two[k] for k in range(n))

    def prepare():
        for b in range(parents):
            for s in range(nlist):
                o = slot_o[b, s]
                for role in roles:
                    pre[role, b * nlist + s] = trn[o + role * last]

    def translate_inner(boxes):
        for b in boxes if inner else ():
            made = {m: [] for m in inner}
            for s in range(nlist):
                o, p = slot_o[b, s], slot_i[b, s]
                for place, m in enumerate(inner):
                    made[m].append((trn[o + m], mid[p + 2 * place], mid[p + 2 * place + 1]))
            for m in inner:
                par[m, b, 0:8, :], par[m, b, 8:16, :] = sums(made[m], 1)

    def translate(role, h):
        src = ends_src(role, h)
        m = ends[role] if thetas > 1 else 0
        if h == 0:
            when_do("left", end_chunk(role, "right"), "wait_recv")
            swap(boxed(src), range(half), 0)
        else:
            when_do("right", end_chunk(role, "left"), "wait_recv")
            swap(boxed(src), range(parents, parents + half), 0)
        for b in range(h * half, (h + 1) * half):
            made = []
            for s in range(nlist):
                p = slot_p[b, s]
                made.append((pre[m, b * nlist + s], src[p], src[p + 1]))
            par[role * last, b, 0:8, :], par[role * last, b, 8:16, :] = sums(made, 2)

    par2 = par.reshape(thetas * parents * pitch(1), LANES)

    def rotate(m, slot, h):
        def part(row):
            return par2[pl.ds((slot * parents + h * half) * pitch(1) + row, half, stride=pitch(1)), :]

        pr = jnp.concatenate([part(2 * i) - part(2 * i + 1) for i in range(4)], axis=1)
        pi = jnp.concatenate([part(8 + 2 * i) + part(9 + 2 * i) for i in range(4)], axis=1)
        for c in range(CHILDREN):
            cc, sc = cos[m, pl.ds(c, 1), :], sin[m, pl.ds(c, 1), :]
            for comp, v in enumerate((pr * cc + pi * sc, pi * cc - pr * sc)):
                rows = pl.ds((2 * h + comp) * some + c * half, half)
                rot_hi[slot, rows, :], rot_lo[slot, rows, :] = split(v)

    def spread(m, slot, i, rows):
        cut = pl.ds(i * LANES, LANES)
        bhi, blo = mat_hi[m, cut, :], mat_lo[m, cut, :]
        y = dot(rot_hi[slot, rows, :], jnp.concatenate([bhi, blo], axis=0), ((1,), (1,)))
        return y[:, :LANES] + (y[:, LANES:] + dot(rot_lo[slot, rows, :], bhi, ((1,), (1,))))

    def spread2(m, slot, i):
        cut = pl.ds(i * LANES, 2 * LANES)
        bhi, blo = mat_hi[m, cut, :], mat_lo[m, cut, :]
        hi = rot_hi[slot]
        y = dot(hi, bhi, ((1,), (1,))) + (dot(hi, blo, ((1,), (1,))) + dot(rot_lo[slot], bhi, ((1,), (1,))))
        return y[:, :LANES], y[:, LANES:]

    def tables():
        shape = (parents, nlist)
        row, slot = lax.broadcasted_iota(jnp.int32, shape, 0), lax.broadcasted_iota(jnp.int32, shape, 1)
        used = jnp.zeros(shape, jnp.int32)
        for b in range(parents):
            used = jnp.where(row == b, count[b], used)
        rows_o[...] = jnp.where(slot < used, rows_o[...], noff) * thetas
        p = rows_p[...] - (x * parents - half)
        near = p - jnp.where(row < half, 0, half)
        idx_rows[...] = jnp.clip(p, 0, 2 * parents - 1) * (pitch(len(inner)) // 8)
        rows_p[...] = jnp.clip(near, 0, ranges - 1) * (pitch(1) // 8)

    idx_rows = slot_i[0]
    tabs = ((rows_p, slot_p), (idx_rows, slot_i[1]), (rows_o, slot_o))
    slot_i = slot_i[1]
    slots = [pltpu.make_async_copy(a, b, fine_sem.at[0]) for a, b in tabs]

    def rim_copy(role, side, h):
        n = 1 if side == "down" else 0
        return remote(rims.at[role, h], got.at[n, h], sent.at[n], rim_recv.at[n], side)

    def rim_out(role, h):
        m = ends[role] * last
        rotate(m, role * last, h)
        rims[role, h] = spread(m, role * last, 2 * ends[role], pl.ds(2 * h * some, 2 * some))
        when_do("down", rim_copy(role, "down", h), "start", ends[role] == 0)
        when_do("up", rim_copy(role, "up", h), "start", ends[role] == 1)

    def halo_in(role, h):
        when_do("down", halo_copy("up", h), "wait_recv", ends[role] == 0)
        when_do("up", halo_copy("down", h), "wait_recv", ends[role] == 1)
        gather(ends[role] * last, [tile(halo, ends[role], (h,))], 2 * ends[role], end_places(role), False, (h,))
        side = ("left", "right")[h]
        when_do(side, end_chunk(role, side), "start")

    with jax.named_scope("k_tables"):
        tables()
    for copy in slots:
        copy.start()
    everything = pl.ds(0, 4 * some)
    with jax.named_scope("k_inner"):
        for place, m in enumerate(inner):
            taps(m)
            where = (flat(mid), pitch(len(inner)), half * pitch(len(inner)) + 16 * place)
            gather(m, [tile(fine, k) for k in (m - 1, m, m + 1)], 0, [where], True)
            for side in ("left", "right"):
                when_do(side, mid_chunk(pl.ds(16 * place, 8), side), "start")
    with jax.named_scope("k_local"):
        for m in sorted({0, last}):
            taps(m)
        for role in roles:
            if thetas == 1:
                gather(0, [tile(fine, 0)], 1, end_places(0)[:1], True)
            else:
                k = ends[role] * (thetas - 2)
                gather(ends[role] * last, [tile(fine, k), tile(fine, k + 1)], 1 - ends[role], end_places(role)[:1], True)
    for copy in slots:
        copy.wait()
    with jax.named_scope("k_trnwait"):
        load.wait()
    with jax.named_scope("k_pre"):
        prepare()
    def first_halos(far):
        for h in (1 - far, far):
            if thetas == 1:
                when_do("down", halo_copy("up", h), "wait_recv")
                when_do("up", halo_copy("down", h), "wait_recv")
                gather(0, [tile(halo, 0, (h,))], 0, end_places(0)[:1], False, (h,))
                gather(0, [tile(halo, 1, (h,))], 2, end_places(0), False, (h,))
                side = ("left", "right")[h]
                when_do(side, end_chunk(0, side), "start")
            else:
                halo_in(0, h)

    def first_end(far):
        for h in (1 - far, far):
            with jax.named_scope("k_tr0_%d" % (h == far)):
                translate(0, h)
            with jax.named_scope("k_rim0_%d" % (h == far)):
                if thetas > 1:
                    rim_out(0, h)
                else:
                    rotate(0, 0, h)
                    for n, side in enumerate(("down", "up")):
                        rims[n, h] = spread(0, 0, 2 * n, pl.ds(2 * h * some, 2 * some))
                        when_do(side, rim_copy(n, side, h), "start")
            if thetas > 1 and h != far:
                with jax.named_scope("k_halo3_0"):
                    halo_in(1, 1 - far)
                with jax.named_scope("k_halo3_1"):
                    halo_in(1, far)

    def second_end(far):
        for h in (1 - far, far):
            with jax.named_scope("k_tr3_%d" % (h == far)):
                translate(1, h)
            with jax.named_scope("k_rim3_%d" % (h == far)):
                rim_out(1, h)

    with jax.named_scope("k_halo0"):
        by_side(first_halos)
    with jax.named_scope("k_boxin12"):
        if inner:
            when_do("right", mid_chunk(pl.ds(0, 8 * len(inner)), "left"), "wait_recv")
            when_do("left", mid_chunk(pl.ds(0, 8 * len(inner)), "right"), "wait_recv")
        for place, m in enumerate(inner):
            swap(boxed(mid, len(inner)), (*range(half), *range(half + parents, 2 * parents)), place)
    with jax.named_scope("k_tr12a"):
        translate_inner(range(half))
    by_side(first_end)
    if thetas == 1:
        acc[0] = spread(0, 0, 1, everything)
    else:
        by_side(second_end)
        with jax.named_scope("k_tr12b"):
            translate_inner(range(half, parents))
        with jax.named_scope("k_spread12"):
            seen = set()

            def put(k, v):
                if k in seen:
                    acc[k] += v
                else:
                    acc[k] = v
                    seen.add(k)

            for m in inner:
                for h in (0, 1):
                    rotate(m, m, h)
                lo, middle = spread2(m, m, 0)
                put(m - 1, lo)
                put(m, middle)
                put(m + 1, spread(m, m, 2, everything))
            for k in range(thetas):
                if k not in seen:
                    acc[k] = jnp.zeros(acc.shape[1:], jnp.float32)
        with jax.named_scope("k_rest"):
            for role in roles:
                k = ends[role] * (thetas - 2)
                lo, hi = spread2(ends[role] * last, role * last, 1 - ends[role])
                acc[k] += lo
                acc[k + 1] += hi

    @pl.when(d == 0)
    def _():
        got[0] = jnp.zeros(got.shape[1:], jnp.float32)

    @pl.when(d == nd - 1)
    def _():
        got[1] = jnp.zeros(got.shape[1:], jnp.float32)

    def result(k):
        for h in (0, 1):
            for comp in range(2):
                for c in range(CHILDREN):
                    at = comp * some + c * half
                    v = acc[k, pl.ds(2 * h * some + at, half), :]
                    if k == 0:
                        v = v + got[0, h, pl.ds(at, half), :]
                    if k == last:
                        v = v + got[1, h, pl.ds(at, half), :]
                    order[k, comp, pl.ds(h * some + c, half, stride=CHILDREN), :] = v
        out[:, :, k * LANES : (k + 1) * LANES] = order[k]

    for k in inner:
        result(k)
    all_sent()
    with jax.named_scope("k_rimB"):
        when_do("down", remote(rims.at[0], got.at[0], sent.at[0], rim_recv.at[0], "up"), "wait_recv")
        when_do("up", remote(rims.at[0], got.at[1], sent.at[1], rim_recv.at[1], "down"), "wait_recv")
    with jax.named_scope("k_end"):
        for k in sorted({0, last}):
            result(k)


VMEM = pl.BlockSpec(memory_space=pltpu.VMEM)
HBM = pl.BlockSpec(memory_space=pltpu.HBM)
MESH = pl.DeviceIdType.MESH


def shards(fine_out, interp_index, interp_weight, child_angle, translator, partners, offsets, list_count):
    _, children, cols = fine_out.shape
    parents = partners.shape[0]
    samples = child_angle.shape[1]
    noff = translator.shape[1]
    tiles = samples // LANES
    thetas = cols // LANES
    f32, bf16 = jnp.float32, jnp.bfloat16
    ordered = translator.reshape(2, noff, tiles, LANES).transpose(1, 2, 0, 3).reshape(noff * thetas, 8, LANES)
    dma = pltpu.SemaphoreType.DMA
    operands = (partners, offsets, list_count, fine_out, interp_index.T, interp_weight.T, child_angle, ordered)
    return pl.pallas_call(
        kernel,
        out_shape=jax.ShapeDtypeStruct((2, children, cols), f32),
        in_specs=[HBM] * 8,
        out_specs=VMEM,
        scratch_shapes=[
            pltpu.SMEM(list_count.shape, jnp.int32),
            pltpu.VMEM(partners.shape, jnp.int32),
            pltpu.VMEM(offsets.shape, jnp.int32),
            pltpu.SMEM(partners.shape, jnp.int32),
            (pltpu.VMEM(partners.shape, jnp.int32), pltpu.SMEM(partners.shape, jnp.int32)),
            pltpu.SMEM(offsets.shape, jnp.int32),
            pltpu.VMEM((thetas, 2, children, LANES), f32),
            pltpu.VMEM((TAPS, samples), jnp.int32),
            pltpu.VMEM((TAPS, samples), f32),
            pltpu.VMEM(child_angle.shape, f32),
            pltpu.VMEM((thetas, CHILDREN, 4 * LANES), f32),
            pltpu.VMEM((thetas, CHILDREN, 4 * LANES), f32),
            dma((2,)),
            pltpu.VMEM((2, 2, children, LANES), f32),
            pltpu.VMEM((thetas, 3 * LANES, 4 * LANES), bf16),
            pltpu.VMEM((thetas, 3 * LANES, 4 * LANES), bf16),
            [pltpu.VMEM((parents * 3 // 2 * pitch(1) // 8, 8, LANES), f32)] * (2 * min(thetas, 2))
            + [pltpu.VMEM((2 * parents * pitch(thetas - 2) // 8, 8, LANES), f32)] * (thetas > 2),
            pltpu.VMEM(((noff + 1) * thetas, 8, LANES), f32),
            pltpu.VMEM((min(thetas, 2), parents * partners.shape[1], 8, LANES), f32),
            pltpu.VMEM((thetas, parents, pitch(1), LANES), f32),
            pltpu.VMEM((thetas, 2 * children, 4 * LANES), bf16),
            pltpu.VMEM((thetas, 2 * children, 4 * LANES), bf16),
            pltpu.VMEM((thetas, 2 * children, LANES), f32),
            pltpu.VMEM((2, 2, children, LANES), f32),
            pltpu.VMEM((2, 2, children, LANES), f32),
            pltpu.VMEM((thetas, 2, children, LANES), f32),
            dma((4,)), dma((2, 2)), dma((6,)), dma((2,)), dma,
        ],
        compiler_params=pltpu.CompilerParams(
            vmem_limit_bytes=40 * 1024 * 1024, collective_id=0, has_side_effects=True
        ),
    )(*(pltpu.with_memory_space_constraint(v, pltpu.HBM) for v in operands))


def solution(mesh):
    placed = (
        P(None, "box", "dir"),
        P("dir", None),
        P("dir", None),
        P(None, "dir"),
        P(None, None, "dir"),
        P("box", None),
        P("box", None),
        P("box"),
    )
    return jax.shard_map(
        shards, mesh=mesh, in_specs=placed, out_specs=P(None, "box", "dir"), check_vma=False
    )
```

```python
import functools

import jax
import jax.numpy as jnp
from jax import lax
from jax.experimental import pallas as pl
from jax.experimental.pallas import tpu as pltpu
from jax.sharding import PartitionSpec as P

LANES = 128
TAPS = 4
CHILDREN = 4


def pitch(rows):
    return 16 * rows + 8


def split(x):
    hi = x.astype(jnp.bfloat16)
    return hi, (x - hi.astype(jnp.float32)).astype(jnp.bfloat16)


def dot(a, b, dims):
    return lax.dot_general(a, b, dimension_numbers=(dims, ((), ())), preferred_element_type=jnp.float32)


def kernel(
    partners_in, offsets_in, count_in, fine_in, idx_in, w_in, angle_in, translator, out,
    count, rows_p, rows_o, slot_p, slot_i, slot_o, fine, idx, w, angle, cos, sin, fine_sem, halo,
    mat_hi, mat_lo, srcs, trn, pre, par, rot_hi, rot_lo, acc, rims, got, order,
    sent, halo_recv, box_recv, rim_recv, trn_sem,
):
    thetas, _, children, _ = fine.shape
    parents = children // CHILDREN
    half = parents // 2
    some = CHILDREN * half
    tiles = angle.shape[1] // LANES
    noff = translator.shape[0] // thetas
    nlist = rows_p.shape[1]
    width = 4 * LANES
    last = thetas - 1
    inner = tuple(range(1, last))
    roles = (0, 1) if thetas > 1 else (0,)
    d, nd = lax.axis_index("dir"), lax.axis_size("dir")
    x, nx = lax.axis_index("box"), lax.axis_size("box")
    has = {"down": d > 0, "up": d < nd - 1, "left": x > 0, "right": x < nx - 1}
    ids = {"down": {"dir": d - 1}, "up": {"dir": d + 1}, "left": {"box": x - 1}, "right": {"box": x + 1}}
    is_even = d % 2 == 0
    top = jnp.where(is_even, 0, 1)
    ends = (top, 1 - top)

    fine_loads = {
        k: pltpu.make_async_copy(fine_in.at[:, :, pl.ds(k * LANES, LANES)], fine.at[k], fine_sem.at[0 if k in (0, last) else 1])
        for k in (*sorted({0, last}), *inner)
    }
    pairs = ((idx_in, idx), (w_in, w), (angle_in, angle), (partners_in, rows_p), (offsets_in, rows_o), (count_in, count))
    loads = [pltpu.make_async_copy(a, b, fine_sem.at[1]) for a, b in pairs]
    for copy in (*fine_loads.values(), *loads):
        copy.start()
    load = pltpu.make_async_copy(translator, trn.at[pl.ds(0, noff * thetas)], trn_sem)
    load.start()

    barrier = pltpu.get_barrier_semaphore()
    for side in ids:
        @pl.when(has[side])
        def _(side=side):
            pl.semaphore_signal(barrier, inc=1, device_id=ids[side], device_id_type=MESH)
    pl.semaphore_wait(barrier, sum(jnp.where(here, 1, 0) for here in has.values()))

    def remote(source, target, send, recv, side):
        return pltpu.make_async_remote_copy(
            src_ref=source, dst_ref=target, send_sem=send, recv_sem=recv,
            device_id=ids[side], device_id_type=MESH,
        )

    def when_do(side, copy, act, also=None):
        @pl.when(has[side] if also is None else jnp.logical_and(has[side], also))
        def _():
            getattr(copy, act)()

    def by_side(body):
        for n in (0, 1):
            @pl.when(x % 2 == n)
            def _(n=n):
                body(n)

    def halo_copy(side, h):
        n, k = (0, last) if side == "up" else (1, 0)
        rows = pl.ds(h * some, some)
        return remote(fine.at[k, :, rows], halo.at[n, :, rows], sent.at[n], halo_recv.at[n, h], side)

    for k in sorted({0, last}):
        fine_loads[k].wait()
    @by_side
    def _(far):
        for h in (1 - far, far):
            for side in ("up", "down"):
                when_do(side, halo_copy(side, h), "start")

    @pl.when(d == 0)
    def _():
        halo[0] = jnp.zeros(halo.shape[1:], jnp.float32)

    @pl.when(d == nd - 1)
    def _():
        halo[1] = jnp.zeros(halo.shape[1:], jnp.float32)

    mid = srcs[2 * len(roles)] if inner else None
    ranges = half + parents

    def boxed(ref, rows=1):
        return ref.reshape(ref.shape[0] * 8 // pitch(rows), pitch(rows), LANES)

    def flat(ref):
        return ref.reshape(ref.shape[0] * 8, LANES)

    def ends_src(role, h):
        return srcs[2 * role + h]

    @pl.when(x == 0)
    def _():
        for role in roles:
            boxed(ends_src(role, 0))[:half] = jnp.zeros((half, pitch(1), LANES), jnp.float32)
        if inner:
            boxed(mid, len(inner))[:half] = jnp.zeros((half, pitch(len(inner)), LANES), jnp.float32)

    @pl.when(x == nx - 1)
    def _():
        for role in roles:
            boxed(ends_src(role, 1))[parents:] = jnp.zeros((half, pitch(1), LANES), jnp.float32)
        if inner:
            boxed(mid, len(inner))[half + parents :] = jnp.zeros((half, pitch(len(inner)), LANES), jnp.float32)

    trn[noff * thetas :] = jnp.zeros((thetas, 8, LANES), jnp.float32)
    for copy in (*loads, *(fine_loads[k] for k in inner)):
        copy.wait()
    first = d * thetas * LANES
    for m in range(thetas):
        cos[m] = jnp.cos(angle[:, m * width : (m + 1) * width])
        sin[m] = jnp.sin(angle[:, m * width : (m + 1) * width])

    def taps(m):
        position = lax.broadcasted_iota(jnp.int32, (3 * LANES, width), 0) + (first + (m - 1) * LANES)
        total = jnp.zeros((3 * LANES, width), jnp.float32)
        for t in range(TAPS):
            at = idx[t : t + 1, m * width : (m + 1) * width]
            total = total + jnp.where(at == position, w[t : t + 1, m * width : (m + 1) * width], 0.0)
        mat_hi[m], mat_lo[m] = split(total)

    def tile(ref, k, halves=(0, 1)):
        return split(jnp.concatenate(
            [
                ref[k, comp, pl.ds(h * some + c, half, stride=CHILDREN), :]
                for h in halves for comp in range(2) for c in range(CHILDREN)
            ],
            axis=0,
        ))

    def gather(m, tiles, start, places, fresh, halves=(0, 1), then=None):
        hi, lo = [v[0] for v in tiles], [v[1] for v in tiles]
        cut = pl.ds(start * LANES, len(tiles) * LANES)
        bhi, blo = mat_hi[m, cut, :], mat_lo[m, cut, :]
        left, right = jnp.concatenate(hi + lo + hi, axis=1), jnp.concatenate([bhi, bhi, blo], axis=0)
        for i in range(4):
            if i % 2 == 0:
                y = dot(left, right[:, i * LANES : (i + 2) * LANES], ((1,), (0,)))
            cut = pl.ds(i * LANES, LANES)
            phases = [(cos[m, pl.ds(c, 1), cut], sin[m, pl.ds(c, 1), cut]) for c in range(CHILDREN)]
            for n, h in enumerate(halves):
                re = im = None
                for c, (cc, sc) in enumerate(phases):
                    at = 2 * n * some + c * half
                    xr = y[at : at + half, i % 2 * LANES : (i % 2 + 1) * LANES]
                    xi = y[at + some : at + some + half, i % 2 * LANES : (i % 2 + 1) * LANES]
                    r, j = xr * cc - xi * sc, xr * sc + xi * cc
                    re, im = (r, j) if c == 0 else (re + r, im + j)

                def own(place, row):
                    return pl.ds(place[2] + h * half * place[1] + 2 * i + row, half, stride=place[1])

                if not fresh:
                    place = places[0]
                    re, im = re + place[0][own(place, 0), :], im + place[0][own(place, 1), :]
                for place in places:
                    for row, v in ((0, re), (1, im), (8, im), (9, re)):
                        place[0][own(place, row), :] = v
            if then and i % 2:
                then(pl.ds(2 * i - 2, 4))

    def end_places(role):
        return [(flat(ends_src(role, 0)), pitch(1), half * pitch(1)), (flat(ends_src(role, 1)), pitch(1), 0)]

    def exchange(source, target, first, rows, sem, side):
        return remote(
            source.at[pl.ds(first, half), rows, :], target[0].at[pl.ds(target[1], half), rows, :],
            sent.at[2 if side == "left" else 3], box_recv.at[sem], side,
        )

    def end_chunk(role, side, rows=pl.ds(0, 8)):
        if side == "left":
            return exchange(boxed(ends_src(role, 1)), (boxed(ends_src(role, 1)), parents), 0, rows, 2 + 2 * role, side)
        return exchange(boxed(ends_src(role, 0)), (boxed(ends_src(role, 0)), 0), parents, rows, 3 + 2 * role, side)

    def mid_chunk(rows, side):
        ref = boxed(mid, len(inner))
        if side == "left":
            return exchange(ref, (ref, half + parents), half, rows, 0, side)
        return exchange(ref, (ref, 0), parents, rows, 1, side)

    def all_sent():
        when_do("up", remote(rims, got, sent.at[0], rim_recv.at[0], "up"), "wait_send")
        when_do("down", remote(rims, got, sent.at[1], rim_recv.at[1], "down"), "wait_send")
        ref, rows = boxed(mid, len(inner)) if inner else boxed(ends_src(0, 0)), pl.ds(0, 8 * thetas)
        for side in ("left", "right"):
            when_do(side, exchange(ref, (ref, half), 0, rows, 0, side), "wait_send")

    even = lax.broadcasted_iota(jnp.int32, (8, LANES), 0) % 2 == 0

    def swap(ref, boxes, place):
        for p in boxes:
            v = ref[p, 16 * place : 16 * place + 8, :]
            ref[p, 16 * place + 8 : 16 * place + 16, :] = jnp.where(even, pltpu.roll(v, 7, 0), pltpu.roll(v, 1, 0))

    def sums(slots, n):
        one, two = {}, {}
        for s, (t, u, v) in enumerate(slots):
            u, v = t * u, t * v
            one[s % n], two[s % n] = (u, v) if s < n else (one[s % n] + u, two[s % n] + v)
        n = min(n, len(one))
        return sum(one[k] for k in range(n)), sum(two[k] for k in range(n))

    def prepare():
        for b in range(parents):
            for s in range(nlist):
                o = slot_o[b, s]
                for role in roles:
                    pre[role, b * nlist + s] = trn[o + role * last]

    def translate_inner(boxes):
        for b in boxes if inner else ():
            made = {m: [] for m in inner}
            for s in range(nlist):
                o, p = slot_o[b, s], slot_i[b, s]
                for place, m in enumerate(inner):
                    made[m].append((trn[o + m], mid[p + 2 * place], mid[p + 2 * place + 1]))
            for m in inner:
                par[m, b, 0:8, :], par[m, b, 8:16, :] = sums(made[m], 1)

    def translate(role, h):
        src = ends_src(role, h)
        m = ends[role] if thetas > 1 else 0
        if h == 0:
            when_do("left", end_chunk(role, "right"), "wait_recv")
            swap(boxed(src), range(half), 0)
        else:
            when_do("right", end_chunk(role, "left"), "wait_recv")
            swap(boxed(src), range(parents, parents + half), 0)
        for b in range(h * half, (h + 1) * half):
            made = []
            for s in range(nlist):
                p = slot_p[b, s]
                made.append((pre[m, b * nlist + s], src[p], src[p + 1]))
            par[role * last, b, 0:8, :], par[role * last, b, 8:16, :] = sums(made, 2)

    par2 = par.reshape(thetas * parents * pitch(1), LANES)

    def rotate(m, slot, h):
        def part(row):
            return par2[pl.ds((slot * parents + h * half) * pitch(1) + row, half, stride=pitch(1)), :]

        pr = jnp.concatenate([part(2 * i) - part(2 * i + 1) for i in range(4)], axis=1)
        pi = jnp.concatenate([part(8 + 2 * i) + part(9 + 2 * i) for i in range(4)], axis=1)
        for c in range(CHILDREN):
            cc, sc = cos[m, pl.ds(c, 1), :], sin[m, pl.ds(c, 1), :]
            for comp, v in enumerate((pr * cc + pi * sc, pi * cc - pr * sc)):
                rows = pl.ds((2 * h + comp) * some + c * half, half)
                rot_hi[slot, rows, :], rot_lo[slot, rows, :] = split(v)

    def spread(m, slot, i, rows):
        cut = pl.ds(i * LANES, LANES)
        bhi, blo = mat_hi[m, cut, :], mat_lo[m, cut, :]
        y = dot(rot_hi[slot, rows, :], jnp.concatenate([bhi, blo], axis=0), ((1,), (1,)))
        return y[:, :LANES] + (y[:, LANES:] + dot(rot_lo[slot, rows, :], bhi, ((1,), (1,))))

    def spread2(m, slot, i):
        cut = pl.ds(i * LANES, 2 * LANES)
        bhi, blo = mat_hi[m, cut, :], mat_lo[m, cut, :]
        hi = rot_hi[slot]
        y = dot(hi, bhi, ((1,), (1,))) + (dot(hi, blo, ((1,), (1,))) + dot(rot_lo[slot], bhi, ((1,), (1,))))
        return y[:, :LANES], y[:, LANES:]

    def tables():
        shape = (parents, nlist)
        row, slot = lax.broadcasted_iota(jnp.int32, shape, 0), lax.broadcasted_iota(jnp.int32, shape, 1)
        used = jnp.zeros(shape, jnp.int32)
        for b in range(parents):
            used = jnp.where(row == b, count[b], used)
        rows_o[...] = jnp.where(slot < used, rows_o[...], noff) * thetas
        p = rows_p[...] - (x * parents - half)
        near = p - jnp.where(row < half, 0, half)
        idx_rows[...] = jnp.clip(p, 0, 2 * parents - 1) * (pitch(len(inner)) // 8)
        rows_p[...] = jnp.clip(near, 0, ranges - 1) * (pitch(1) // 8)

    idx_rows = slot_i[0]
    tabs = ((rows_p, slot_p), (idx_rows, slot_i[1]), (rows_o, slot_o))
    slot_i = slot_i[1]
    slots = [pltpu.make_async_copy(a, b, fine_sem.at[0]) for a, b in tabs]

    def rim_copy(role, side, h):
        n = 1 if side == "down" else 0
        return remote(rims.at[role, h], got.at[n, h], sent.at[n], rim_recv.at[n], side)

    def rim_out(role, h):
        m = ends[role] * last
        rotate(m, role * last, h)
        rims[role, h] = spread(m, role * last, 2 * ends[role], pl.ds(2 * h * some, 2 * some))
        when_do("down", rim_copy(role, "down", h), "start", ends[role] == 0)
        when_do("up", rim_copy(role, "up", h), "start", ends[role] == 1)

    def halo_in(role, h):
        when_do("down", halo_copy("up", h), "wait_recv", ends[role] == 0)
        when_do("up", halo_copy("down", h), "wait_recv", ends[role] == 1)
        side = ("left", "right")[h]

        def send(rows):
            when_do(side, end_chunk(role, side, rows), "start")

        gather(ends[role] * last, [tile(halo, ends[role], (h,))], 2 * ends[role], end_places(role), False, (h,), send)

    with jax.named_scope("k_tables"):
        tables()
    for copy in slots:
        copy.start()
    everything = pl.ds(0, 4 * some)
    with jax.named_scope("k_inner"):
        for place, m in enumerate(inner):
            taps(m)
            where = (flat(mid), pitch(len(inner)), half * pitch(len(inner)) + 16 * place)
            gather(m, [tile(fine, k) for k in (m - 1, m, m + 1)], 0, [where], True)
            for side in ("left", "right"):
                when_do(side, mid_chunk(pl.ds(16 * place, 8), side), "start")
    with jax.named_scope("k_local"):
        for m in sorted({0, last}):
            taps(m)
        for role in roles:
            if thetas == 1:
                gather(0, [tile(fine, 0)], 1, end_places(0)[:1], True)
            else:
                k = ends[role] * (thetas - 2)
                gather(ends[role] * last, [tile(fine, k), tile(fine, k + 1)], 1 - ends[role], end_places(role)[:1], True)
    for copy in slots:
        copy.wait()
    with jax.named_scope("k_trnwait"):
        load.wait()
    with jax.named_scope("k_pre"):
        prepare()
    def first_halos(far):
        for h in (1 - far, far):
            if thetas == 1:
                when_do("down", halo_copy("up", h), "wait_recv")
                when_do("up", halo_copy("down", h), "wait_recv")
                gather(0, [tile(halo, 0, (h,))], 0, end_places(0)[:1], False, (h,))
                gather(0, [tile(halo, 1, (h,))], 2, end_places(0), False, (h,))
                side = ("left", "right")[h]
                when_do(side, end_chunk(0, side), "start")
            else:
                halo_in(0, h)

    def first_end(far):
        for h in (1 - far, far):
            with jax.named_scope("k_tr0_%d" % (h == far)):
                translate(0, h)
            with jax.named_scope("k_rim0_%d" % (h == far)):
                if thetas > 1:
                    rim_out(0, h)
                else:
                    rotate(0, 0, h)
                    for n, side in enumerate(("down", "up")):
                        rims[n, h] = spread(0, 0, 2 * n, pl.ds(2 * h * some, 2 * some))
                        when_do(side, rim_copy(n, side, h), "start")
            if thetas > 1 and h != far:
                with jax.named_scope("k_halo3_0"):
                    halo_in(1, 1 - far)
                with jax.named_scope("k_halo3_1"):
                    halo_in(1, far)

    def second_end(far):
        for h in (1 - far, far):
            with jax.named_scope("k_tr3_%d" % (h == far)):
                translate(1, h)
            with jax.named_scope("k_rim3_%d" % (h == far)):
                rim_out(1, h)

    with jax.named_scope("k_halo0"):
        by_side(first_halos)
    with jax.named_scope("k_boxin12"):
        if inner:
            when_do("right", mid_chunk(pl.ds(0, 8 * len(inner)), "left"), "wait_recv")
            when_do("left", mid_chunk(pl.ds(0, 8 * len(inner)), "right"), "wait_recv")
        for place, m in enumerate(inner):
            swap(boxed(mid, len(inner)), (*range(half), *range(half + parents, 2 * parents)), place)
    with jax.named_scope("k_tr12a"):
        translate_inner(range(half))
    by_side(first_end)
    if thetas == 1:
        acc[0] = spread(0, 0, 1, everything)
    else:
        by_side(second_end)
        with jax.named_scope("k_tr12b"):
            translate_inner(range(half, parents))
        with jax.named_scope("k_spread12"):
            seen = set()

            def put(k, v):
                if k in seen:
                    acc[k] += v
                else:
                    acc[k] = v
                    seen.add(k)

            for m in inner:
                for h in (0, 1):
                    rotate(m, m, h)
                lo, middle = spread2(m, m, 0)
                put(m - 1, lo)
                put(m, middle)
                put(m + 1, spread(m, m, 2, everything))
            for k in range(thetas):
                if k not in seen:
                    acc[k] = jnp.zeros(acc.shape[1:], jnp.float32)
        with jax.named_scope("k_rest"):
            for role in roles:
                k = ends[role] * (thetas - 2)
                lo, hi = spread2(ends[role] * last, role * last, 1 - ends[role])
                acc[k] += lo
                acc[k + 1] += hi

    @pl.when(d == 0)
    def _():
        got[0] = jnp.zeros(got.shape[1:], jnp.float32)

    @pl.when(d == nd - 1)
    def _():
        got[1] = jnp.zeros(got.shape[1:], jnp.float32)

    def result(k):
        for h in (0, 1):
            for comp in range(2):
                for c in range(CHILDREN):
                    at = comp * some + c * half
                    v = acc[k, pl.ds(2 * h * some + at, half), :]
                    if k == 0:
                        v = v + got[0, h, pl.ds(at, half), :]
                    if k == last:
                        v = v + got[1, h, pl.ds(at, half), :]
                    order[k, comp, pl.ds(h * some + c, half, stride=CHILDREN), :] = v
        out[:, :, k * LANES : (k + 1) * LANES] = order[k]

    for k in inner:
        result(k)
    all_sent()
    with jax.named_scope("k_rimB"):
        when_do("down", remote(rims.at[0], got.at[0], sent.at[0], rim_recv.at[0], "up"), "wait_recv")
        when_do("up", remote(rims.at[0], got.at[1], sent.at[1], rim_recv.at[1], "down"), "wait_recv")
    with jax.named_scope("k_end"):
        for k in sorted({0, last}):
            result(k)


VMEM = pl.BlockSpec(memory_space=pltpu.VMEM)
HBM = pl.BlockSpec(memory_space=pltpu.HBM)
MESH = pl.DeviceIdType.MESH


def shards(fine_out, interp_index, interp_weight, child_angle, translator, partners, offsets, list_count):
    _, children, cols = fine_out.shape
    parents = partners.shape[0]
    samples = child_angle.shape[1]
    noff = translator.shape[1]
    tiles = samples // LANES
    thetas = cols // LANES
    f32, bf16 = jnp.float32, jnp.bfloat16
    ordered = translator.reshape(2, noff, tiles, LANES).transpose(1, 2, 0, 3).reshape(noff * thetas, 8, LANES)
    dma = pltpu.SemaphoreType.DMA
    operands = (partners, offsets, list_count, fine_out, interp_index.T, interp_weight.T, child_angle, ordered)
    return pl.pallas_call(
        kernel,
        out_shape=jax.ShapeDtypeStruct((2, children, cols), f32),
        in_specs=[HBM] * 8,
        out_specs=VMEM,
        scratch_shapes=[
            pltpu.SMEM(list_count.shape, jnp.int32),
            pltpu.VMEM(partners.shape, jnp.int32),
            pltpu.VMEM(offsets.shape, jnp.int32),
            pltpu.SMEM(partners.shape, jnp.int32),
            (pltpu.VMEM(partners.shape, jnp.int32), pltpu.SMEM(partners.shape, jnp.int32)),
            pltpu.SMEM(offsets.shape, jnp.int32),
            pltpu.VMEM((thetas, 2, children, LANES), f32),
            pltpu.VMEM((TAPS, samples), jnp.int32),
            pltpu.VMEM((TAPS, samples), f32),
            pltpu.VMEM(child_angle.shape, f32),
            pltpu.VMEM((thetas, CHILDREN, 4 * LANES), f32),
            pltpu.VMEM((thetas, CHILDREN, 4 * LANES), f32),
            dma((2,)),
            pltpu.VMEM((2, 2, children, LANES), f32),
            pltpu.VMEM((thetas, 3 * LANES, 4 * LANES), bf16),
            pltpu.VMEM((thetas, 3 * LANES, 4 * LANES), bf16),
            [pltpu.VMEM((parents * 3 // 2 * pitch(1) // 8, 8, LANES), f32)] * (2 * min(thetas, 2))
            + [pltpu.VMEM((2 * parents * pitch(thetas - 2) // 8, 8, LANES), f32)] * (thetas > 2),
            pltpu.VMEM(((noff + 1) * thetas, 8, LANES), f32),
            pltpu.VMEM((min(thetas, 2), parents * partners.shape[1], 8, LANES), f32),
            pltpu.VMEM((thetas, parents, pitch(1), LANES), f32),
            pltpu.VMEM((thetas, 2 * children, 4 * LANES), bf16),
            pltpu.VMEM((thetas, 2 * children, 4 * LANES), bf16),
            pltpu.VMEM((thetas, 2 * children, LANES), f32),
            pltpu.VMEM((2, 2, children, LANES), f32),
            pltpu.VMEM((2, 2, children, LANES), f32),
            pltpu.VMEM((thetas, 2, children, LANES), f32),
            dma((4,)), dma((2, 2)), dma((6,)), dma((2,)), dma,
        ],
        compiler_params=pltpu.CompilerParams(
            vmem_limit_bytes=40 * 1024 * 1024, collective_id=0, has_side_effects=True
        ),
    )(*(pltpu.with_memory_space_constraint(v, pltpu.HBM) for v in operands))


def solution(mesh):
    placed = (
        P(None, "box", "dir"),
        P("dir", None),
        P("dir", None),
        P(None, "dir"),
        P(None, None, "dir"),
        P("box", None),
        P("box", None),
        P("box"),
    )
    return jax.shard_map(
        shards, mesh=mesh, in_specs=placed, out_specs=P(None, "box", "dir"), check_vma=False
    )
```
